768 devices in a mesh: dp: 12 (over z_lo, x), spatial: 64 (over y, z_hi, core).
Axes of the slice: x: 4, y: 8, z: 12 (z_hi: 4, z_lo: 3; z = z_hi * 3 + z_lo), core: 2. Of those that a mesh axis runs over, the one named last changes fastest.
Arguments:
- volume: bfloat16 [12, 128, 16, 8, 128], P('dp', 'spatial'), may hold values from -16 to 16
- cotangent: bfloat16 [12, 128, 16, 8, 128], P('dp', 'spatial'), may hold values from -6 to 6
- master: float32 [3456, 128], P('dp'), may hold values from -0.109375 to 0.109375
- moment: float32 [3456, 128], P('dp'), may hold values from -6 to 6
- second: float32 [3456, 128], P('dp'), may hold values from 0.25 to 4
Outputs:
- activation: bfloat16 [12, 128, 16, 8, 128], P('dp', 'spatial')
- input_grad: bfloat16 [12, 128, 16, 8, 128], P('dp', 'spatial')
- master_next: float32 [3456, 128], P('dp')
- moment_next: float32 [3456, 128], P('dp')
- second_next: float32 [3456, 128], P('dp')
The draws below stay inside these ranges and needn't reach their ends.
All inputs are finite; a program needn't handle non-finite values.
Results may differ from the reference program's by a relative error of at most 0.002.
The reference program's roundings to bfloat16 on the way (of `kernel` and `hidden_grad`) count: a program that leaves them out, or rounds other values in their place, can miss the bound.
Values may be sent and summed in bfloat16 or wider, within the bound.
No kernel may reach another device: no remote copies, remote signals or barrier semaphores. Data moves between devices by JAX's collectives and lax.ppermute only.
A program may use at most 64 MiB of HBM per device.

```python
import math
import jax
import jax.numpy as jnp
from jax import lax

C = 128
TAPS = 27
NY = 16
NX = 8
NZ = 128
BATCH = 12


def spiked(drawn, rng, source, target, shards_of, factor):
    owner, partner = [(jnp.arange(drawn.shape[axis_at]) // (drawn.shape[axis_at] // shards_of)).reshape([-1 if axis == axis_at else 1 for axis in range(drawn.ndim)]) for axis_at in (source, target)]
    chosen = jax.random.permutation(rng, shards_of)[partner]
    strong = (owner == chosen) | (owner == (partner + shards_of // 2) % shards_of)
    return jnp.where(strong, factor * drawn, drawn)


def levels(rng, extent, shards, least, largest):
    level, own = 1.0, jax.random.fold_in(rng, 6)
    for dim, shards_of in shards:
        steps = jnp.exp(jax.random.uniform(jax.random.fold_in(own, dim), (shards_of,), jnp.float32, least / len(shards), largest / len(shards)))
        level = level * jnp.repeat(steps, extent[dim] // shards_of).reshape([-1 if axis == dim else 1 for axis in range(len(extent))])
    return level


def centred(own_key, dims, scale, bound, pieces=(), kind=jnp.bfloat16):
    loudness = levels(own_key, dims, pieces, -0.22, 0.18) if pieces else 1.0
    array = jax.random.normal(own_key, dims, jnp.float32) * scale * loudness
    return jnp.minimum(jnp.maximum(array, -bound), bound).astype(kind)


def heavy_noise(own_key, extent, scale, bound, cuts, heavy, kind=jnp.bfloat16):
    drawn = scale * jax.random.normal(own_key, extent, jnp.float32)
    if cuts:
        drawn = drawn * levels(own_key, extent, cuts, -0.22, 0.18)
    return jnp.clip(spiked(drawn, jax.random.fold_in(own_key, 3), *heavy), -bound, bound).astype(kind)


def setup_inputs(seed: int = 0) -> dict:
    seeds = jax.random.split(jax.random.key(seed), 6)
    volume = heavy_noise(seeds[0], (BATCH, NZ, NY, NX, C), 1.0, 16.0, ((0, 12), (1, 64)), (1, 4, 64, 4.0))
    cotangent = centred(seeds[1], (BATCH, NZ, NY, NX, C), 1.0, 6.0, ((0, 12), (1, 64)))
    master = centred(seeds[2], (TAPS * C, C), (TAPS * C) ** -0.5, 0.109375, ((0, 12),), jnp.float32)
    moment = centred(seeds[3], (TAPS * C, C), 1.0, 6.0, ((0, 12),), jnp.float32)
    second = jnp.clip(jnp.exp(math.log(4.0) - 2.7725887 * jax.random.uniform(seeds[4], (TAPS * C, C), jnp.float32) ** levels(seeds[4], (TAPS * C, C), ((0, 12),), -0.2, 0.2)), 0.25, 4.0)
    return {"volume": volume, "cotangent": cotangent, "master": master, "moment": moment, "second": second}


def convolve(inputs, weights):
    return lax.conv_general_dilated(inputs, weights, (1, 1, 1), 'SAME', dimension_numbers=('NDHWC', 'DHWIO', 'NDHWC'), precision=lax.Precision.HIGHEST)

def reference(volume, cotangent, master, moment, second):
    width = master.shape[1]
    rounded = lax.optimization_barrier(master.astype(jnp.bfloat16))
    kernel = rounded.astype(jnp.float32).reshape(3, 3, 3, width, width)
    field = volume.astype(jnp.float32)
    preact, pullback = jax.vjp(convolve, field, kernel)
    activation = jax.nn.silu(preact).astype(jnp.bfloat16)
    sigma = jax.nn.sigmoid(preact)
    slope = sigma * (1.0 + preact * (1.0 - sigma))
    hidden_grad = lax.optimization_barrier((cotangent.astype(jnp.float32) * slope).astype(jnp.bfloat16))
    input_full, weight_full = pullback(hidden_grad.astype(jnp.float32))
    input_grad = input_full.astype(jnp.bfloat16)
    weight_grad = weight_full.reshape(27 * width, width) / math.sqrt(BATCH * NZ * NY * NX)
    moment_next = 0.9 * moment + 0.1 * weight_grad
    second_next = 0.999 * second + 0.001 * weight_grad * weight_grad
    master_next = master - 0.001 * (moment_next / (jnp.sqrt(second_next) + 1e-08) + 0.01 * master)
    return (activation, input_grad, master_next, moment_next, second_next)
```

```python
import math

import jax
import jax.numpy as jnp
from jax import lax
from jax.sharding import PartitionSpec as P


def copy_for_each(value, axis):
    count = lax.axis_size(axis)
    return lax.all_to_all(
        jnp.broadcast_to(value[None], (count, *value.shape)), axis, 0, 0, tiled=True
    )


def joined_along(tiles, dim):
    tiles = jnp.moveaxis(tiles, 0, dim)
    dims = tiles.shape
    return tiles.reshape(*dims[:dim], dims[dim] * dims[dim + 1], *dims[dim + 2 :])


def gather_directly(value, axis, dim):
    tiles = copy_for_each(value, axis)
    return joined_along(tiles, dim)


def with_halo(block, sides, width):
    for axis, dim in sides:
        count = lax.axis_size(axis)
        forward = [(i, i + 1) for i in range(count - 1)]
        backward = [(target, source) for source, target in forward]
        low = lax.ppermute(
            lax.slice_in_dim(block, block.shape[dim] - width, None, axis=dim), axis, forward
        )
        high = lax.ppermute(lax.slice_in_dim(block, 0, width, axis=dim), axis, backward)
        block = jnp.concatenate([low, block, high], axis=dim)
    return block


def in_blocks(value, dim, count):
    before, after = (value.shape[:dim], value.shape[dim + 1 :])
    return jnp.moveaxis(value.reshape(*before, count, -1, *after), dim, 0)


def sum_at_owner(value, axis, dim):
    tiles = in_blocks(value, dim, lax.axis_size(axis))
    arrived = lax.all_to_all(tiles, axis, split_axis=0, concat_axis=0, tiled=True)
    return arrived.astype(jnp.float32).sum(axis=0)


def exchanged(tiles, axis, groups):
    return lax.all_to_all(tiles, axis, 0, 0, tiled=True, axis_index_groups=groups)


def total_of_pieces(value, axis):
    count = lax.axis_size(axis)
    inner = 8
    outer = count // inner
    same_inner = [[o * inner + i for o in range(outer)] for i in range(inner)]
    same_outer = [[o * inner + i for i in range(inner)] for o in range(outer)]
    pieces = value.reshape(outer, -1, value.shape[-1])
    piece = exchanged(pieces, axis, same_inner).sum(0)
    piece = exchanged(jnp.broadcast_to(piece[None], (inner, *piece.shape)), axis, same_outer).sum(0)
    whole = exchanged(jnp.broadcast_to(piece[None], (outer, *piece.shape)), axis, same_inner)
    return whole.reshape(value.shape)


def silu_slope(preact):
    sigma = jax.nn.sigmoid(preact)
    return sigma * (1.0 + preact * (1.0 - sigma))


def pad_sides(field):
    return jnp.pad(field, ((0, 0), (1, 1), (1, 1), (0, 0)))


def forward_taps(padded, kernel, planes, rows, cols):
    width = kernel.shape[1]
    total = jnp.zeros((planes * rows * cols, width), jnp.float32)
    for offset_z in range(3):
        for offset_y in range(3):
            for offset_x in range(3):
                tap_index = offset_z * 9 + offset_y * 3 + offset_x
                piece = padded[
                    offset_z : offset_z + planes,
                    offset_y : offset_y + rows,
                    offset_x : offset_x + cols,
                ].reshape(-1, width)
                total = total + jnp.dot(
                    piece, kernel[tap_index], preferred_element_type=jnp.float32
                )
    return total


def backward_taps(grad_pad, kernel, planes, rows, cols):
    width = kernel.shape[1]
    total = jnp.zeros((planes * rows * cols, width), jnp.float32)
    for offset_z in range(3):
        for offset_y in range(3):
            for offset_x in range(3):
                tap_index = offset_z * 9 + offset_y * 3 + offset_x
                piece = grad_pad[
                    2 - offset_z : 2 - offset_z + planes,
                    2 - offset_y : 2 - offset_y + rows,
                    2 - offset_x : 2 - offset_x + cols,
                ].reshape(-1, width)
                total = total + lax.dot_general(
                    piece,
                    kernel[tap_index],
                    (((1,), (1,)), ((), ())),
                    preferred_element_type=jnp.float32,
                )
    return total


def weight_taps(padded, hidden_grad, planes, rows, cols):
    width = hidden_grad.shape[1]
    blocks = []
    for offset_z in range(3):
        for offset_y in range(3):
            for offset_x in range(3):
                piece = padded[
                    offset_z : offset_z + planes,
                    offset_y : offset_y + rows,
                    offset_x : offset_x + cols,
                ].reshape(-1, width)
                blocks.append(
                    lax.dot_general(
                        piece,
                        hidden_grad,
                        (((0,), (0,)), ((), ())),
                        preferred_element_type=jnp.float32,
                    )
                )
    return jnp.concatenate(blocks, axis=0)


def per_device(volume, cotangent, master, moment, second):
    planes = volume.shape[1]
    rows = volume.shape[2]
    cols = volume.shape[3]
    width = volume.shape[4]
    kernel = gather_directly(master.astype(jnp.bfloat16), "dp", 0).reshape(27, width, width)
    wide = with_halo(volume, (("spatial", 1),), 1)[0]
    padded = pad_sides(wide)
    preact = forward_taps(padded, kernel, planes, rows, cols)
    activated = jax.nn.silu(preact).astype(jnp.bfloat16)
    hidden_grad = (cotangent[0].reshape(-1, width).astype(jnp.float32) * silu_slope(preact)).astype(
        jnp.bfloat16
    )
    grad_block = hidden_grad.reshape(1, planes, rows, cols, width)
    wide_grad = with_halo(grad_block, (("spatial", 1),), 1)[0]
    grad_pad = pad_sides(wide_grad)
    input_grad = backward_taps(grad_pad, kernel, planes, rows, cols).astype(jnp.bfloat16)
    local_grad = weight_taps(padded, hidden_grad, planes, rows, cols)
    partial_grad = sum_at_owner(local_grad.astype(jnp.bfloat16), "dp", 0)
    shard = total_of_pieces(partial_grad, "spatial")
    cells_all = lax.axis_size("dp") * lax.axis_size("spatial") * planes * rows * cols
    weight_grad = shard / math.sqrt(cells_all)
    moment_next = 0.9 * moment + 0.1 * weight_grad
    second_next = 0.999 * second + 0.001 * weight_grad * weight_grad
    master_next = master - 0.001 * (moment_next / (jnp.sqrt(second_next) + 1e-08) + 0.01 * master)
    activation = activated.reshape(1, planes, rows, cols, width)
    input_block = input_grad.reshape(1, planes, rows, cols, width)
    return (activation, input_block, master_next, moment_next, second_next)


def solution(mesh):
    return jax.shard_map(
        per_device,
        mesh=mesh,
        in_specs=(
            P("dp", "spatial", None, None, None),
            P("dp", "spatial", None, None, None),
            P("dp", None),
            P("dp", None),
            P("dp", None),
        ),
        out_specs=(
            P("dp", "spatial", None, None, None),
            P("dp", "spatial", None, None, None),
            P("dp", None),
            P("dp", None),
            P("dp", None),
        ),
        check_vma=False,
    )
```

```python
import functools
import math

import jax
import jax.numpy as jnp
from jax import lax
from jax.experimental import pallas as pl
from jax.experimental.pallas import tpu as pltpu
from jax.sharding import PartitionSpec as P

F32 = jnp.float32
BF16 = jnp.bfloat16
OUTER = 8
MIDDLE = 4
PAIR = 2
HALF = 64
PIECE = 24


def core_is_low():
    return lax.rem(lax.axis_index("spatial"), PAIR) == 0


def lane_of(shape):
    return lax.broadcasted_iota(jnp.int32, shape, len(shape) - 1)


def pick(low, when_low, when_high):
    return jnp.where(low, when_low, when_high)


def pack_body(master_ref, volume_ref, send_ref, edge_ref):
    low = core_is_low()
    rows = master_ref.shape[0] // 2
    top = master_ref[:rows]
    bottom = master_ref[rows:]
    first = pick(low, top, pltpu.roll(top, HALF, 1))
    second = pick(low, pltpu.roll(bottom, HALF, 1), bottom)
    packed = jnp.where(lane_of(top.shape) < HALF, first, second).astype(BF16)
    for owner in range(send_ref.shape[0]):
        send_ref[owner] = packed
    edge_ref[...] = pick(low, volume_ref[0, 0].astype(F32), volume_ref[0, 1].astype(F32)).astype(BF16)


def shifted(plane, dy, dx):
    rows, cols, width = plane.shape
    if dx:
        at = lax.broadcasted_iota(jnp.int32, plane.shape, 1)
        keep = at < cols - 1 if dx > 0 else at > 0
        plane = jnp.where(keep, pltpu.roll(plane, (-dx) % cols, 1), 0.0)
    if dy:
        gap = jnp.zeros((1, cols, width), plane.dtype)
        plane = jnp.concatenate([plane[1:], gap] if dy > 0 else [gap, plane[:-1]], axis=0)
    return plane


def write_windows(window_ref, planes, sign):
    cells = planes[0].shape[0] * planes[0].shape[1]
    width = planes[0].shape[2]
    for index, plane in enumerate(planes):
        for dx in (-1, 0, 1):
            column = shifted(plane, 0, dx)
            for dy in (-1, 0, 1):
                tap = (sign * dy + 1) * 3 + sign * dx + 1
                window_ref[index * cells : (index + 1) * cells, tap * width : (tap + 1) * width] = (
                    shifted(column, dy, 0).reshape(cells, width).astype(BF16)
                )


def forward_body(
    kernel_ref,
    volume_ref,
    beside_ref,
    far_ref,
    near_ref,
    cot_ref,
    cot_beside_ref,
    half_kernel_ref,
    own_act_ref,
    swap_ref,
    near_grad_ref,
    far_grad_ref,
    weight_ref,
    window_ref,
    turned_ref,
    total_ref,
):
    low = core_is_low()
    owners, rows, width = kernel_ref.shape
    mask = (lane_of((rows, width)) < HALF) == low
    for owner in range(owners):
        packed = kernel_ref[owner].astype(F32)
        rolled = pltpu.roll(packed, HALF, 1)
        base = owner * 2 * rows
        half_kernel_ref[base : base + rows] = jnp.where(mask, pick(low, packed, rolled), 0.0).astype(BF16)
        half_kernel_ref[base + rows : base + 2 * rows] = jnp.where(
            mask, pick(low, rolled, packed), 0.0
        ).astype(BF16)
    own = [volume_ref[0, i].astype(F32) for i in range(2)]
    beside = [beside_ref[0, i].astype(F32) for i in range(2)]
    far = far_ref[...].astype(F32)
    near = near_ref[...].astype(F32)
    planes = [pick(low, near, far)]
    planes += [pick(low, own[i], beside[i]) for i in range(2)]
    planes += [pick(low, beside[i], own[i]) for i in range(2)]
    planes += [pick(low, far, near)]
    write_windows(window_ref, planes, 1)
    cells = planes[0].shape[0] * planes[0].shape[1]
    count = 4 * cells
    span = 9 * width
    preact = jnp.zeros((count, width), F32)
    for a in range(3):
        preact = preact + jnp.dot(
            window_ref[a * cells : a * cells + count],
            half_kernel_ref[a * span : (a + 1) * span],
            preferred_element_type=F32,
        )
    sigma = jax.nn.sigmoid(preact)
    slope = sigma * (1.0 + preact * (1.0 - sigma))
    activation = (preact * sigma).astype(BF16)
    cot_own = cot_ref[0].astype(F32).reshape(2 * cells, width)
    cot_beside = cot_beside_ref[0].astype(F32).reshape(2 * cells, width)
    cotangent = jnp.concatenate(
        [pick(low, cot_own, cot_beside), pick(low, cot_beside, cot_own)], axis=0
    )
    wide_mask = (lane_of((count, width)) < HALF) == low
    grad = jnp.where(wide_mask, cotangent * slope, 0.0)
    rounded = grad.astype(BF16)
    swap_ref[:count] = rounded
    act_low = activation[: 2 * cells]
    act_high = activation[2 * cells :]
    own_act_ref[...] = pick(low, act_low.astype(F32), act_high.astype(F32)).astype(BF16)
    swap_ref[count:] = pick(low, act_high.astype(F32), act_low.astype(F32)).astype(BF16)
    first = grad[:cells]
    last = grad[3 * cells :]
    near_grad_ref[...] = pick(low, first, last).astype(BF16)
    far_grad_ref[...] = pick(low, last, first).astype(BF16)
    turned_ref[...] = grad.T.astype(BF16)
    mine = pick(low, turned_ref[:HALF].astype(F32), turned_ref[HALF:].astype(F32)).astype(BF16)
    for a in range(3):
        total_ref[:, a * span : (a + 1) * span] = jnp.dot(
            mine, window_ref[a * cells : a * cells + count], preferred_element_type=F32
        )
    lane = lane_of((HALF, width))

    def columns(start):
        tile, offset = divmod(start, width)
        here = total_ref[:, tile * width : (tile + 1) * width]
        if not offset:
            return here
        here = pltpu.roll(here, width - offset, 1)
        if (tile + 1) * width >= total_ref.shape[1]:
            return here
        after = pltpu.roll(total_ref[:, (tile + 1) * width : (tile + 2) * width], width - offset, 1)
        return jnp.where(lane < width - offset, here, after)

    shard = 2 * rows
    rest = shard - 2 * width
    folds = width // rest
    group = HALF // folds
    for owner in range(owners):
        start = owner * shard
        weight_ref[owner, :HALF] = columns(start).astype(BF16)
        weight_ref[owner, HALF : 2 * HALF] = columns(start + width).astype(BF16)
        tail = columns(start + 2 * width)
        folded = tail[:group]
        for fold in range(1, folds):
            part = pltpu.roll(tail[fold * group : (fold + 1) * group], fold * rest, 1)
            folded = jnp.where(lane[:group] >= fold * rest, part, folded)
        weight_ref[owner, 2 * HALF :] = folded.astype(BF16)


def backward_body(
    mine_ref, other_ref, own_ref, got_ref, near_ref, far_ref, act_ref, out_act_ref, out_ref, window_ref
):
    low = core_is_low()
    cells, width = near_ref.shape
    shape = out_ref.shape[2:]
    count = 4 * cells
    full = own_ref[:count].astype(F32) + got_ref[:count].astype(F32)
    edge = (near_ref[...].astype(F32) + far_ref[...].astype(F32)).reshape(shape)
    grads = [full[i * cells : (i + 1) * cells].reshape(shape) for i in range(4)]
    planes = [pick(low, edge, grads[1]), pick(low, grads[0], grads[2])]
    planes += [pick(low, grads[1], grads[3]), pick(low, grads[2], edge)]
    write_windows(window_ref, planes, -1)
    total = jnp.zeros((2 * cells, width), F32)
    for a in range(3):
        for e in range(9):
            tap = a * 9 + e
            weight = mine_ref[tap * width : (tap + 1) * width] + other_ref[tap * width : (tap + 1) * width]
            total = total + lax.dot_general(
                window_ref[(2 - a) * cells : (4 - a) * cells, e * width : (e + 1) * width],
                weight,
                (((1,), (1,)), ((), ())),
                preferred_element_type=F32,
            )
    out_ref[0] = total.reshape(2, *shape).astype(BF16)
    activation = act_ref[...].astype(F32) + got_ref[count:].astype(F32)
    lane_low = (lane_of(activation.shape) < HALF) == low
    activation = jnp.where(lane_low, act_ref[...].astype(F32), got_ref[count:].astype(F32))
    out_act_ref[0] = activation.reshape(2, *shape).astype(BF16)


def update_body(cells_all, grads_ref, master_ref, moment_ref, second_ref, out_ref, out_m_ref, out_s_ref, grad_ref):
    rows, width = master_ref.shape
    pieces = rows // 2 // PIECE
    halves = []
    for half in range(PAIR):
        halves.append(
            jnp.concatenate([grads_ref[PAIR * i + half] for i in range(pieces)], axis=0)
        )
    rest = rows - 2 * width
    folds = width // rest
    group = HALF // folds
    for part in range(2):
        both = jnp.concatenate([h[part * HALF : (part + 1) * HALF] for h in halves], axis=0)
        grad_ref[part * width : (part + 1) * width] = both.T
    tails = []
    for h in halves:
        tail = h[2 * HALF :]
        for fold in range(folds):
            tails.append(pltpu.roll(tail, width - fold * rest, 1) if fold else tail)
    assert len(tails) * group == width
    grad_ref[2 * width :] = jnp.concatenate(tails, axis=0).T[:rest]
    weight_grad = grad_ref[...] / math.sqrt(cells_all)
    moment_next = 0.9 * moment_ref[...] + 0.1 * weight_grad
    second_next = 0.999 * second_ref[...] + 0.001 * weight_grad * weight_grad
    master = master_ref[...]
    out_ref[...] = master - 0.001 * (moment_next / (jnp.sqrt(second_next) + 1e-08) + 0.01 * master)
    out_m_ref[...] = moment_next
    out_s_ref[...] = second_next


def exchanged(tiles, groups):
    return lax.all_to_all(tiles, "spatial", 0, 0, tiled=True, axis_index_groups=groups)


def moved(value, perm):
    return lax.ppermute(value, "spatial", perm)


def per_device(volume, cotangent, master, moment, second):
    _, planes, rows, cols, width = volume.shape
    cells = rows * cols
    owners = lax.axis_size("dp")
    count = lax.axis_size("spatial")
    shard = master.shape[0]
    taps_all = owners * shard
    like = jax.ShapeDtypeStruct

    def inside(pairs):
        return [(i, j) for i, j in pairs if 0 <= j < count]

    swap = [(i, i ^ 1) for i in range(count)]
    near = inside((i, i - 1 if i % 2 == 0 else i + 1) for i in range(count))
    far_out = inside((i, i - 2 if i % 2 == 0 else i + 2) for i in range(count))
    far_in = inside((i, i + 2 if i % 2 == 0 else i - 2) for i in range(count))

    send, edge = pl.pallas_call(
        pack_body,
        out_shape=(like((owners, shard // 2, width), BF16), like((rows, cols, width), BF16)),
        name="pack",
    )(master, volume)
    halves = lax.all_to_all(send, "dp", 0, 0, tiled=True)
    far_plane = moved(edge, far_out)
    near_plane = moved(edge, near)
    beside = moved(volume, swap)
    cot_beside = moved(cotangent, swap)
    half_kernel, own_act, swapped, near_grad, far_grad, weight = pl.pallas_call(
        forward_body,
        out_shape=(
            like((taps_all, width), BF16),
            like((2 * cells, width), BF16),
            like((6 * cells, width), BF16),
            like((cells, width), BF16),
            like((cells, width), BF16),
            like((owners, shard // 2, width), BF16),
        ),
        scratch_shapes=[
            pltpu.VMEM((6 * cells, 9 * width), BF16),
            pltpu.VMEM((width, 4 * cells), BF16),
            pltpu.VMEM((HALF, taps_all), F32),
        ],
        name="forward",
    )(halves, volume, beside, far_plane, near_plane, cotangent, cot_beside)
    arrived = lax.all_to_all(weight, "dp", 0, 0, tiled=True)

    got = moved(swapped, swap)
    near_got = moved(near_grad, near)
    far_got = moved(far_grad, far_in)
    other_kernel = moved(half_kernel, swap)
    activation, input_grad = pl.pallas_call(
        backward_body,
        out_shape=(like(volume.shape, BF16), like(volume.shape, BF16)),
        scratch_shapes=[pltpu.VMEM((4 * cells, 9 * width), BF16)],
        cost_estimate=pl.CostEstimate(
            flops=2 * 2 * cells * taps_all * width, bytes_accessed=4 * taps_all * width, transcendentals=0
        ),
        name="backward",
    )(half_kernel, other_kernel, swapped, got, near_got, far_got, own_act)

    same_y = [
        [(y * MIDDLE + h) * PAIR + c for h in range(MIDDLE)] for y in range(OUTER) for c in range(PAIR)
    ]
    same_rest = [[y * MIDDLE * PAIR + r for y in range(OUTER)] for r in range(MIDDLE * PAIR)]
    same_z = [
        [(y * MIDDLE + h) * PAIR + c for y in range(OUTER) for c in range(PAIR)] for h in range(MIDDLE)
    ]
    pieces = shard // 2 // PIECE
    summed = arrived.astype(F32).sum(axis=0).reshape(pieces, PIECE, width)
    summed = jnp.pad(summed, ((0, OUTER - pieces), (0, 0), (0, 0)))
    piece = exchanged(summed, same_rest).sum(0)
    piece = exchanged(jnp.broadcast_to(piece[None], (MIDDLE, PIECE, width)), same_y).sum(0)
    joined = exchanged(jnp.broadcast_to(piece[None], (OUTER * PAIR, PIECE, width)), same_z)
    cells_all = owners * count * planes * cells
    state = like(master.shape, F32)
    master_next, moment_next, second_next = pl.pallas_call(
        functools.partial(update_body, cells_all),
        out_shape=(state, state, state),
        scratch_shapes=[pltpu.VMEM(master.shape, F32)],
        name="update",
    )(joined, master, moment, second)
    return (activation, input_grad, master_next, moment_next, second_next)


def solution(mesh):
    return jax.shard_map(
        per_device,
        mesh=mesh,
        in_specs=(
            P("dp", "spatial", None, None, None),
            P("dp", "spatial", None, None, None),
            P("dp", None),
            P("dp", None),
            P("dp", None),
        ),
        out_specs=(
            P("dp", "spatial", None, None, None),
            P("dp", "spatial", None, None, None),
            P("dp", None),
            P("dp", None),
            P("dp", None),
        ),
        check_vma=False,
    )
```

```python
import functools
import math

import jax
import jax.numpy as jnp
from jax import lax
from jax.experimental import pallas as pl
from jax.experimental.pallas import tpu as pltpu
from jax.sharding import PartitionSpec as P

F32 = jnp.float32
BF16 = jnp.bfloat16
OUTER = 8
MIDDLE = 4
PAIR = 2
HALF = 64
PIECE = 24


def core_is_low():
    return lax.rem(lax.axis_index("spatial"), PAIR) == 0


def lane_of(shape):
    return lax.broadcasted_iota(jnp.int32, shape, len(shape) - 1)


def pick(low, when_low, when_high):
    return jnp.where(low, when_low, when_high)


def pack_body(master_ref, volume_ref, cot_ref, send_ref, edge_ref, slab_ref):
    low = core_is_low()
    rows = master_ref.shape[0] // 2
    top = master_ref[:rows]
    bottom = master_ref[rows:]
    first = pick(low, top, pltpu.roll(top, HALF, 1))
    second = pick(low, pltpu.roll(bottom, HALF, 1), bottom)
    packed = jnp.where(lane_of(top.shape) < HALF, first, second).astype(BF16)
    for owner in range(send_ref.shape[0]):
        send_ref[owner] = packed
    edge_ref[...] = pick(low, volume_ref[0, 0].astype(F32), volume_ref[0, 1].astype(F32)).astype(BF16)
    slab_ref[:2] = volume_ref[0]
    slab_ref[2:] = cot_ref[0]


def shifted(plane, dy, dx):
    _, cols, width = plane.shape
    if dx:
        at = lax.broadcasted_iota(jnp.int32, plane.shape, 1)
        keep = at < cols - 1 if dx > 0 else at > 0
        plane = jnp.where(keep, pltpu.roll(plane, (-dx) % cols, 1), 0.0)
    if dy:
        gap = jnp.zeros((1, cols, width), plane.dtype)
        plane = jnp.concatenate([plane[1:], gap] if dy > 0 else [gap, plane[:-1]], axis=0)
    return plane


def tap_pieces(plane, sign):
    columns = [shifted(plane, 0, sign * (f - 1)) for f in range(3)]
    return [shifted(columns[f], sign * (e - 1), 0) for e in range(3) for f in range(3)]


def forward_body(
    kernel_ref,
    volume_ref,
    cot_ref,
    beside_ref,
    far_ref,
    near_ref,
    act_ref,
    grad_ref,
    first_ref,
    last_ref,
    weight_ref,
    window_ref,
    wide_ref,
    turned_ref,
    stack_ref,
    total_ref,
):
    low = core_is_low()
    owners, rows, width = kernel_ref.shape
    own = [volume_ref[0, i].astype(F32) for i in range(2)]
    beside = [beside_ref[i].astype(F32) for i in range(2)]
    far = far_ref[...].astype(F32)
    near = near_ref[...].astype(F32)
    planes = [pick(low, near, far)]
    planes += [pick(low, own[i], beside[i]) for i in range(2)]
    planes += [pick(low, beside[i], own[i]) for i in range(2)]
    planes += [pick(low, far, near)]
    cells = planes[0].shape[0] * planes[0].shape[1]
    for index, plane in enumerate(planes):
        for tap, piece in enumerate(tap_pieces(plane, 1)):
            window_ref[index * cells : (index + 1) * cells, tap * width : (tap + 1) * width] = (
                piece.reshape(cells, width).astype(BF16)
            )
    mask = (lane_of((rows, width)) < HALF) == low
    group = owners // 3
    for j in range(group):
        base = j * 2 * rows
        ends = []
        for offset in range(3):
            packed = kernel_ref[offset * group + j].astype(F32)
            rolled = pltpu.roll(packed, HALF, 1)
            ends.append((pick(low, packed, rolled), pick(low, rolled, packed)))
        for k in range(2):
            at = slice(base + k * rows, base + (k + 1) * rows)
            wide_ref[at, :width] = jnp.where(mask, ends[0][k], ends[1][1 - k]).astype(BF16)
            wide_ref[at, width:] = jnp.where(mask, ends[2][k], 0.0).astype(BF16)
    count = 4 * cells
    span = 9 * width
    product = jnp.dot(window_ref[...], wide_ref[...], preferred_element_type=F32)
    wide_mask = (lane_of((count, width)) < HALF) == low
    preact = product[:count, :width] + product[2 * cells :, width:]
    preact = preact + pltpu.roll(product[cells : cells + count, :width], HALF, 1)
    preact = jnp.where(wide_mask, preact, 0.0)
    sigma = jax.nn.sigmoid(preact)
    slope = sigma * (1.0 + preact * (1.0 - sigma))
    act_ref[...] = (preact * sigma).astype(BF16)
    cot_own = cot_ref[0].astype(F32).reshape(2 * cells, width)
    cot_beside = beside_ref[2:].astype(F32).reshape(2 * cells, width)
    cotangent = jnp.concatenate(
        [pick(low, cot_own, cot_beside), pick(low, cot_beside, cot_own)], axis=0
    )
    grad = jnp.where(wide_mask, cotangent * slope, 0.0)
    rounded = grad.astype(BF16)
    grad_ref[...] = rounded
    first_ref[...] = rounded[:cells]
    last_ref[...] = rounded[3 * cells :]
    turned_ref[...] = grad.T
    mine = pick(low, turned_ref[:HALF], turned_ref[HALF:]).astype(BF16)
    stack_ref[...] = jnp.zeros_like(stack_ref)
    for offset in range(3):
        stack_ref[offset * HALF : (offset + 1) * HALF, offset * cells : offset * cells + count] = mine
    stacked = jnp.dot(stack_ref[...], window_ref[...], preferred_element_type=F32)
    for offset in range(3):
        total_ref[:, offset * span : (offset + 1) * span] = stacked[offset * HALF : (offset + 1) * HALF]
    lane = lane_of((HALF, width))

    def columns(start):
        tile, offset = divmod(start, width)
        here = total_ref[:, tile * width : (tile + 1) * width]
        if not offset:
            return here
        here = pltpu.roll(here, width - offset, 1)
        if (tile + 1) * width >= total_ref.shape[1]:
            return here
        after = pltpu.roll(total_ref[:, (tile + 1) * width : (tile + 2) * width], width - offset, 1)
        return jnp.where(lane < width - offset, here, after)

    shard = 2 * rows
    rest = shard - 2 * width
    folds = width // rest
    lines = HALF // folds
    for owner in range(owners):
        start = owner * shard
        weight_ref[owner, :HALF] = columns(start).astype(BF16)
        weight_ref[owner, HALF : 2 * HALF] = columns(start + width).astype(BF16)
        tail = columns(start + 2 * width)
        folded = tail[:lines]
        for fold in range(1, folds):
            part = pltpu.roll(tail[fold * lines : (fold + 1) * lines], fold * rest, 1)
            folded = jnp.where(lane[:lines] >= fold * rest, part, folded)
        weight_ref[owner, 2 * HALF :] = folded.astype(BF16)


def backward_body(
    kernel_ref, grad_ref, before_ref, after_ref, act_ref, own_ref, swap_ref, here_ref, there_ref, turn_ref, window_ref
):
    low = core_is_low()
    owners, rows, width = kernel_ref.shape
    cells = before_ref.shape[0]
    count = 4 * cells
    shape = (cells // 8, 8, width)
    mask = (lane_of((rows, width)) < HALF) == low
    for owner in range(owners):
        packed = kernel_ref[owner].astype(F32)
        rolled = pltpu.roll(packed, HALF, 1)
        one, two = pick(low, packed, rolled), pick(low, rolled, packed)
        base = owner * 2 * rows
        for ref, top, bottom, keep in ((here_ref, one, two, mask), (there_ref, two, one, ~mask)):
            ref[base : base + rows] = jnp.where(keep, top, 0.0).astype(BF16)
            ref[base + rows : base + 2 * rows] = jnp.where(keep, bottom, 0.0).astype(BF16)
    for offset in range(3):
        for pair in range(5):
            tap = offset * 9 + 2 * pair
            weight = here_ref[tap * width : (tap + 1) * width]
            if pair < 4:
                weight = weight + there_ref[(tap + 1) * width : (tap + 2) * width]
            turn_ref[offset, :, pair * width : (pair + 1) * width] = weight
    planes = [before_ref[...]] + [grad_ref[i * cells : (i + 1) * cells] for i in range(4)] + [after_ref[...]]
    for index, plane in enumerate(planes):
        pieces = tap_pieces(plane.astype(F32).reshape(shape), -1)
        for pair in range(5):
            piece = pieces[2 * pair].reshape(cells, width)
            if pair < 4:
                piece = piece + pltpu.roll(pieces[2 * pair + 1].reshape(cells, width), HALF, 1)
            window_ref[index * cells : (index + 1) * cells, pair * width : (pair + 1) * width] = piece.astype(
                BF16
            )
    total = jnp.zeros((count, width), F32)
    for offset in range(3):
        total = total + lax.dot_general(
            window_ref[(2 - offset) * cells : (2 - offset) * cells + count],
            turn_ref[offset],
            (((1,), (1,)), ((), ())),
            preferred_element_type=F32,
        )
    half = count // 2
    own_ref[...] = pick(low, total[:half], total[half:])
    swap_ref[:half] = pick(low, total[half:], total[:half])
    act = act_ref[...].astype(F32)
    swap_ref[half:] = pick(low, act[half:], act[:half])


def finish_body(own_ref, act_ref, got_ref, out_act_ref, out_ref):
    low = core_is_low()
    half, _ = own_ref.shape
    shape = out_ref.shape[1:]
    out_ref[0] = (own_ref[...] + got_ref[:half]).reshape(shape).astype(BF16)
    act = act_ref[...].astype(F32)
    mine = pick(low, act[:half], act[half:])
    mask = (lane_of(mine.shape) < HALF) == low
    out_act_ref[0] = jnp.where(mask, mine, got_ref[half:]).reshape(shape).astype(BF16)


def update_body(cells_all, grads_ref, master_ref, moment_ref, second_ref, out_ref, out_m_ref, out_s_ref, grad_ref):
    rows, width = master_ref.shape
    pieces = rows // 2 // PIECE
    halves = []
    for half in range(PAIR):
        halves.append(
            jnp.concatenate([grads_ref[PAIR * i + half] for i in range(pieces)], axis=0)
        )
    rest = rows - 2 * width
    folds = width // rest
    group = HALF // folds
    for part in range(2):
        both = jnp.concatenate([h[part * HALF : (part + 1) * HALF] for h in halves], axis=0)
        grad_ref[part * width : (part + 1) * width] = both.T
    tails = []
    for h in halves:
        tail = h[2 * HALF :]
        for fold in range(folds):
            tails.append(pltpu.roll(tail, width - fold * rest, 1) if fold else tail)
    assert len(tails) * group == width
    grad_ref[2 * width :] = jnp.concatenate(tails, axis=0).T[:rest]
    weight_grad = grad_ref[...] / math.sqrt(cells_all)
    moment_next = 0.9 * moment_ref[...] + 0.1 * weight_grad
    second_next = 0.999 * second_ref[...] + 0.001 * weight_grad * weight_grad
    master = master_ref[...]
    out_ref[...] = master - 0.001 * (moment_next / (jnp.sqrt(second_next) + 1e-08) + 0.01 * master)
    out_m_ref[...] = moment_next
    out_s_ref[...] = second_next


def exchanged(tiles, groups):
    return lax.all_to_all(tiles, "spatial", 0, 0, tiled=True, axis_index_groups=groups)


def moved(value, perm):
    return lax.ppermute(value, "spatial", perm)


def layer(volume, cotangent, master, moment, second):
    _, planes, rows, cols, width = volume.shape
    cells = rows * cols
    owners = lax.axis_size("dp")
    count = lax.axis_size("spatial")
    shard = master.shape[0]
    taps_all = owners * shard
    like = jax.ShapeDtypeStruct

    def inside(pairs):
        return [(i, j) for i, j in pairs if 0 <= j < count]

    swap = [(i, i ^ 1) for i in range(count)]
    near = inside((i, i - 1 if i % 2 == 0 else i + 1) for i in range(count))
    far = inside((i, i - 2 if i % 2 == 0 else i + 2) for i in range(count))
    onward = inside((i, i + 2) for i in range(count))
    backward = inside((i, i - 2) for i in range(count))

    send, edge, slab = pl.pallas_call(
        pack_body,
        out_shape=(
            like((owners, shard // 2, width), BF16),
            like((rows, cols, width), BF16),
            like((4, rows, cols, width), BF16),
        ),
        name="pack",
    )(master, volume, cotangent)
    halves = lax.all_to_all(send, "dp", 0, 0, tiled=True)
    far_plane = moved(edge, far)
    near_plane = moved(edge, near)
    beside = moved(slab, swap)
    cell_half = like((cells, width), BF16)
    cell_all = like((4 * cells, width), BF16)
    act, grad, first, last, weight = pl.pallas_call(
        forward_body,
        out_shape=(cell_all, cell_all, cell_half, cell_half, like((owners, shard // 2, width), BF16)),
        scratch_shapes=[
            pltpu.VMEM((6 * cells, 9 * width), BF16),
            pltpu.VMEM((9 * width, 2 * width), BF16),
            pltpu.VMEM((width, 4 * cells), F32),
            pltpu.VMEM((3 * HALF, 6 * cells), BF16),
            pltpu.VMEM((HALF, taps_all), F32),
        ],
        name="forward",
    )(halves, volume, cotangent, beside, far_plane, near_plane)
    arrived = lax.all_to_all(weight, "dp", 0, 0, tiled=True)
    before = moved(last, onward)
    after = moved(first, backward)
    own, swapped = pl.pallas_call(
        backward_body,
        out_shape=(like((2 * cells, width), F32), like((4 * cells, width), F32)),
        scratch_shapes=[
            pltpu.VMEM((taps_all, width), BF16),
            pltpu.VMEM((taps_all, width), BF16),
            pltpu.VMEM((3, width, 5 * width), BF16),
            pltpu.VMEM((6 * cells, 5 * width), BF16),
        ],
        cost_estimate=pl.CostEstimate(
            flops=2 * 2 * cells * taps_all * width, bytes_accessed=taps_all * width, transcendentals=0
        ),
        name="backward",
    )(halves, grad, before, after, act)
    got = moved(swapped, swap)
    activation, input_grad = pl.pallas_call(
        finish_body, out_shape=(like(volume.shape, BF16), like(volume.shape, BF16)), name="finish"
    )(own, act, got)

    same_y = [
        [(y * MIDDLE + h) * PAIR + c for h in range(MIDDLE)] for y in range(OUTER) for c in range(PAIR)
    ]
    same_rest = [[y * MIDDLE * PAIR + r for y in range(OUTER)] for r in range(MIDDLE * PAIR)]
    same_z = [
        [(y * MIDDLE + h) * PAIR + c for y in range(OUTER) for c in range(PAIR)] for h in range(MIDDLE)
    ]
    pieces = shard // 2 // PIECE
    summed = arrived.astype(F32).sum(axis=0).reshape(pieces, PIECE, width)
    summed = jnp.pad(summed, ((0, OUTER - pieces), (0, 0), (0, 0)))
    piece = exchanged(summed, same_rest)
    piece = piece.sum(0)
    piece = exchanged(jnp.broadcast_to(piece[None], (MIDDLE, PIECE, width)), same_y)
    piece = piece.sum(0)
    joined = exchanged(jnp.broadcast_to(piece[None], (OUTER * PAIR, PIECE, width)), same_z)
    cells_all = owners * count * planes * cells
    state = like(master.shape, F32)
    master_next, moment_next, second_next = pl.pallas_call(
        functools.partial(update_body, cells_all),
        out_shape=(state, state, state),
        scratch_shapes=[pltpu.VMEM(master.shape, F32)],
        name="update",
    )(joined, master, moment, second)
    return (activation, input_grad, master_next, moment_next, second_next)


def solution(mesh):
    return jax.shard_map(
        layer,
        mesh=mesh,
        in_specs=(
            P("dp", "spatial", None, None, None),
            P("dp", "spatial", None, None, None),
            P("dp", None),
            P("dp", None),
            P("dp", None),
        ),
        out_specs=(
            P("dp", "spatial", None, None, None),
            P("dp", "spatial", None, None, None),
            P("dp", None),
            P("dp", None),
            P("dp", None),
        ),
        check_vma=False,
    )
```

```python
import functools
import math

import jax
import jax.numpy as jnp
from jax import lax
from jax.experimental import pallas as pl
from jax.experimental.pallas import tpu as pltpu
from jax.sharding import PartitionSpec as P

F32 = jnp.float32
BF16 = jnp.bfloat16
OUTER = 8
MIDDLE = 4
PAIR = 2
HALF = 64
PIECE = 24


def core_is_low():
    return lax.rem(lax.axis_index("spatial"), PAIR) == 0


def lane_of(shape):
    return lax.broadcasted_iota(jnp.int32, shape, len(shape) - 1)


def pick(low, when_low, when_high):
    return jnp.where(low, when_low, when_high)


def pack_body(master_ref, volume_ref, cot_ref, send_ref, near_ref, slab_ref):
    low = core_is_low()
    rows = master_ref.shape[0] // 2
    top = master_ref[:rows]
    bottom = master_ref[rows:]
    first = pick(low, top, pltpu.roll(top, HALF, 1))
    second = pick(low, pltpu.roll(bottom, HALF, 1), bottom)
    packed = jnp.where(lane_of(top.shape) < HALF, first, second).astype(BF16)
    for owner in range(send_ref.shape[0]):
        send_ref[owner] = packed
    near_ref[:2] = volume_ref[0]
    near_ref[2] = pick(low, cot_ref[0, 0].astype(F32), cot_ref[0, 1].astype(F32)).astype(BF16)
    slab_ref[:2] = volume_ref[0]
    slab_ref[2:] = cot_ref[0]


def shifted(plane, dy, dx):
    _, cols, width = plane.shape
    if dx:
        at = lax.broadcasted_iota(jnp.int32, plane.shape, 1)
        keep = at < cols - 1 if dx > 0 else at > 0
        plane = jnp.where(keep, pltpu.roll(plane, (-dx) % cols, 1), 0.0)
    if dy:
        gap = jnp.zeros((1, cols, width), plane.dtype)
        plane = jnp.concatenate([plane[1:], gap] if dy > 0 else [gap, plane[:-1]], axis=0)
    return plane


def tap_pieces(plane, sign):
    columns = [shifted(plane, 0, sign * (f - 1)) for f in range(3)]
    return [shifted(columns[f], sign * (e - 1), 0) for e in range(3) for f in range(3)]


def kernel_rows(low, mine, other):
    mine = mine.astype(F32)
    other = other.astype(F32)
    left = pick(low, mine, other)
    right = pick(low, other, mine)
    keep = lane_of(left.shape) < HALF
    first = jnp.where(keep, left, pltpu.roll(right, HALF, 1))
    second = jnp.where(keep, pltpu.roll(left, HALF, 1), right)
    return first.astype(BF16), second.astype(BF16)


def windows_body(volume_ref, cot_ref, beside_ref, near_ref, far_ref, window_ref, all_cot_ref):
    low = core_is_low()
    own = [volume_ref[0, i].astype(F32) for i in range(2)]
    beside = [beside_ref[i].astype(F32) for i in range(2)]
    near = [near_ref[i].astype(F32) for i in range(3)]
    far = [far_ref[i].astype(F32) for i in range(3)]
    planes = [pick(low, near[i], far[i]) for i in range(2)]
    planes += [pick(low, own[i], beside[i]) for i in range(2)]
    planes += [pick(low, beside[i], own[i]) for i in range(2)]
    planes += [pick(low, far[i], near[i]) for i in range(2)]
    cells = planes[0].shape[0] * planes[0].shape[1]
    width = planes[0].shape[2]
    for index, plane in enumerate(planes):
        for tap, piece in enumerate(tap_pieces(plane, 1)):
            window_ref[index * cells : (index + 1) * cells, tap * width : (tap + 1) * width] = (
                piece.reshape(cells, width).astype(BF16)
            )
    cot_own = cot_ref[0].astype(F32).reshape(2 * cells, width)
    cot_beside = beside_ref[2:].astype(F32).reshape(2 * cells, width)
    near_cot = near[2].reshape(cells, width)
    far_cot = far[2].reshape(cells, width)
    parts = [
        pick(low, near_cot, far_cot),
        pick(low, cot_own, cot_beside),
        pick(low, cot_beside, cot_own),
        pick(low, far_cot, near_cot),
    ]
    all_cot_ref[...] = jnp.concatenate(parts, axis=0).astype(BF16)


def forward_body(
    kernel_ref,
    other_ref,
    window_ref,
    cot_ref,
    out_act_ref,
    grad_ref,
    weight_ref,
    wide_ref,
    deep_ref,
    turned_ref,
    stack_ref,
    total_ref,
):
    low = core_is_low()
    owners, rows, width = kernel_ref.shape
    cells = cot_ref.shape[0] // 6
    group = owners // 3
    for owner in range(owners):
        offset, j = divmod(owner, group)
        blocks = kernel_rows(low, kernel_ref[owner], other_ref[owner])
        for k in range(2):
            at = slice((2 * j + k) * rows, (2 * j + k + 1) * rows)
            if offset < 2:
                wide_ref[at, offset * width : (offset + 1) * width] = blocks[k]
            else:
                deep_ref[at] = blocks[k]
    count = 6 * cells
    inner = 4 * cells
    span = 9 * width
    product = jnp.dot(window_ref[: count + cells], wide_ref[...], preferred_element_type=F32)
    preact = jnp.dot(window_ref[2 * cells :], deep_ref[...], preferred_element_type=F32)
    preact = preact + product[:count, :width] + product[cells:, width:]
    sigma = jax.nn.sigmoid(preact)
    slope = sigma * (1.0 + preact * (1.0 - sigma))
    act = preact[cells : cells + inner] * sigma[cells : cells + inner]
    act = pick(low, act[: inner // 2], act[inner // 2 :])
    out_act_ref[0] = act.reshape(out_act_ref.shape[1:]).astype(BF16)
    grad = cot_ref[...].astype(F32) * slope
    grad_ref[...] = pick(low, grad[:inner], grad[2 * cells :]).astype(BF16)
    turned_ref[...] = grad[cells : cells + inner].T
    mine = pick(low, turned_ref[:HALF], turned_ref[HALF:]).astype(BF16)
    stack_ref[...] = jnp.zeros_like(stack_ref)
    for offset in range(3):
        stack_ref[offset * HALF : (offset + 1) * HALF, offset * cells : offset * cells + inner] = mine
    stacked = jnp.dot(stack_ref[...], window_ref[cells : cells + count], preferred_element_type=F32)
    for offset in range(3):
        total_ref[:, offset * span : (offset + 1) * span] = stacked[offset * HALF : (offset + 1) * HALF]
    lane = lane_of((HALF, width))

    def columns(start):
        tile, offset = divmod(start, width)
        here = total_ref[:, tile * width : (tile + 1) * width]
        if not offset:
            return here
        here = pltpu.roll(here, width - offset, 1)
        if (tile + 1) * width >= total_ref.shape[1]:
            return here
        after = pltpu.roll(total_ref[:, (tile + 1) * width : (tile + 2) * width], width - offset, 1)
        return jnp.where(lane < width - offset, here, after)

    shard = 2 * rows
    rest = shard - 2 * width
    folds = width // rest
    lines = HALF // folds
    for owner in range(owners):
        start = owner * shard
        weight_ref[owner, :HALF] = columns(start).astype(BF16)
        weight_ref[owner, HALF : 2 * HALF] = columns(start + width).astype(BF16)
        tail = columns(start + 2 * width)
        folded = tail[:lines]
        for fold in range(1, folds):
            part = pltpu.roll(tail[fold * lines : (fold + 1) * lines], fold * rest, 1)
            folded = jnp.where(lane[:lines] >= fold * rest, part, folded)
        weight_ref[owner, 2 * HALF :] = folded.astype(BF16)


def backward_body(kernel_ref, other_ref, grad_ref, out_ref, window_ref, turn_ref):
    low = core_is_low()
    owners, rows, width = kernel_ref.shape
    shape = out_ref.shape[2:]
    cells = grad_ref.shape[0] // 4
    for owner in range(owners):
        blocks = kernel_rows(low, kernel_ref[owner], other_ref[owner])
        for k in range(2):
            turn_ref[(2 * owner + k) * rows : (2 * owner + k + 1) * rows] = blocks[k]
    for index in range(4):
        plane = grad_ref[index * cells : (index + 1) * cells].astype(F32).reshape(shape)
        for tap, piece in enumerate(tap_pieces(plane, -1)):
            window_ref[index * cells : (index + 1) * cells, tap * width : (tap + 1) * width] = (
                piece.reshape(cells, width).astype(BF16)
            )
    total = jnp.zeros((2 * cells, width), F32)
    for offset in range(3):
        for tap in range(9):
            at = (offset * 9 + tap) * width
            total = total + lax.dot_general(
                window_ref[(2 - offset) * cells : (4 - offset) * cells, tap * width : (tap + 1) * width],
                turn_ref[at : at + width],
                (((1,), (1,)), ((), ())),
                preferred_element_type=F32,
            )
    out_ref[0] = total.reshape(2, *shape).astype(BF16)


def update_body(cells_all, grads_ref, master_ref, moment_ref, second_ref, out_ref, out_m_ref, out_s_ref, grad_ref):
    rows, width = master_ref.shape
    pieces = rows // 2 // PIECE
    halves = []
    for half in range(PAIR):
        halves.append(
            jnp.concatenate([grads_ref[PAIR * i + half] for i in range(pieces)], axis=0)
        )
    rest = rows - 2 * width
    folds = width // rest
    group = HALF // folds
    for part in range(2):
        both = jnp.concatenate([h[part * HALF : (part + 1) * HALF] for h in halves], axis=0)
        grad_ref[part * width : (part + 1) * width] = both.T
    tails = []
    for h in halves:
        tail = h[2 * HALF :]
        for fold in range(folds):
            tails.append(pltpu.roll(tail, width - fold * rest, 1) if fold else tail)
    assert len(tails) * group == width
    grad_ref[2 * width :] = jnp.concatenate(tails, axis=0).T[:rest]
    weight_grad = grad_ref[...] / math.sqrt(cells_all)
    moment_next = 0.9 * moment_ref[...] + 0.1 * weight_grad
    second_next = 0.999 * second_ref[...] + 0.001 * weight_grad * weight_grad
    master = master_ref[...]
    out_ref[...] = master - 0.001 * (moment_next / (jnp.sqrt(second_next) + 1e-08) + 0.01 * master)
    out_m_ref[...] = moment_next
    out_s_ref[...] = second_next


def exchanged(tiles, groups):
    return lax.all_to_all(tiles, "spatial", 0, 0, tiled=True, axis_index_groups=groups)


def moved(value, perm):
    return lax.ppermute(value, "spatial", perm)


def layer(volume, cotangent, master, moment, second):
    _, planes, rows, cols, width = volume.shape
    cells = rows * cols
    owners = lax.axis_size("dp")
    count = lax.axis_size("spatial")
    shard = master.shape[0]
    taps_all = owners * shard
    like = jax.ShapeDtypeStruct

    def inside(pairs):
        return [(i, j) for i, j in pairs if 0 <= j < count]

    swap = [(i, i ^ 1) for i in range(count)]
    outward = inside((i, i - 1 if i % 2 == 0 else i + 1) for i in range(count))

    packed = like((owners, shard // 2, width), BF16)
    send, edge, slab = pl.pallas_call(
        pack_body,
        out_shape=(packed, like((3, rows, cols, width), BF16), like((4, rows, cols, width), BF16)),
        name="pack",
    )(master, volume, cotangent)
    halves = lax.all_to_all(send, "dp", 0, 0, tiled=True)
    near = moved(edge, outward)
    beside = moved(slab, swap)
    far = moved(near, swap)
    window, all_cot = pl.pallas_call(
        windows_body,
        out_shape=(like((8 * cells, 9 * width), BF16), like((6 * cells, width), BF16)),
        name="windows",
    )(volume, cotangent, beside, near, far)
    others = moved(halves, swap)
    activation, grad, weight = pl.pallas_call(
        forward_body,
        out_shape=(like(volume.shape, BF16), like((4 * cells, width), BF16), packed),
        scratch_shapes=[
            pltpu.VMEM((9 * width, 2 * width), BF16),
            pltpu.VMEM((9 * width, width), BF16),
            pltpu.VMEM((width, 4 * cells), F32),
            pltpu.VMEM((3 * HALF, 6 * cells), BF16),
            pltpu.VMEM((HALF, taps_all), F32),
        ],
        name="forward",
    )(halves, others, window, all_cot)
    arrived = lax.all_to_all(weight, "dp", 0, 0, tiled=True)
    input_grad = pl.pallas_call(
        backward_body,
        out_shape=like(volume.shape, BF16),
        scratch_shapes=[
            pltpu.VMEM((4 * cells, 9 * width), BF16),
            pltpu.VMEM((taps_all, width), BF16),
        ],
        cost_estimate=pl.CostEstimate(
            flops=2 * 2 * cells * taps_all * width, bytes_accessed=taps_all * width, transcendentals=0
        ),
        name="backward",
    )(halves, others, grad)

    same_y = [
        [(y * MIDDLE + h) * PAIR + c for h in range(MIDDLE)] for y in range(OUTER) for c in range(PAIR)
    ]
    same_rest = [[y * MIDDLE * PAIR + r for y in range(OUTER)] for r in range(MIDDLE * PAIR)]
    same_z = [
        [(y * MIDDLE + h) * PAIR + c for y in range(OUTER) for c in range(PAIR)] for h in range(MIDDLE)
    ]
    pieces = shard // 2 // PIECE
    summed = arrived.astype(F32).sum(axis=0).reshape(pieces, PIECE, width)
    summed = jnp.pad(summed, ((0, OUTER - pieces), (0, 0), (0, 0)))
    piece = exchanged(summed, same_rest)
    piece = piece.sum(0)
    piece = exchanged(jnp.broadcast_to(piece[None], (MIDDLE, PIECE, width)), same_y)
    piece = piece.sum(0)
    joined = exchanged(jnp.broadcast_to(piece[None], (OUTER * PAIR, PIECE, width)), same_z)
    cells_all = owners * count * planes * cells
    state = like(master.shape, F32)
    master_next, moment_next, second_next = pl.pallas_call(
        functools.partial(update_body, cells_all),
        out_shape=(state, state, state),
        scratch_shapes=[pltpu.VMEM(master.shape, F32)],
        name="update",
    )(joined, master, moment, second)
    return (activation, input_grad, master_next, moment_next, second_next)


def solution(mesh):
    return jax.shard_map(
        layer,
        mesh=mesh,
        in_specs=(
            P("dp", "spatial", None, None, None),
            P("dp", "spatial", None, None, None),
            P("dp", None),
            P("dp", None),
            P("dp", None),
        ),
        out_specs=(
            P("dp", "spatial", None, None, None),
            P("dp", "spatial", None, None, None),
            P("dp", None),
            P("dp", None),
            P("dp", None),
        ),
        check_vma=False,
    )
```

```python
import functools
import math

import jax
import jax.numpy as jnp
from jax import lax
from jax.experimental import pallas as pl
from jax.experimental.pallas import tpu as pltpu
from jax.sharding import PartitionSpec as P

F32 = jnp.float32
BF16 = jnp.bfloat16
OUTER = 8
MIDDLE = 4
PAIR = 2
HALF = 64
PIECE = 24


def core_is_low():
    return lax.rem(lax.axis_index("spatial"), PAIR) == 0


def lane_of(shape):
    return lax.broadcasted_iota(jnp.int32, shape, len(shape) - 1)


def pick(low, when_low, when_high):
    return jnp.where(low, when_low, when_high)


def pack_body(master_ref, volume_ref, cot_ref, send_ref, near_ref, slab_ref):
    low = core_is_low()
    rows = master_ref.shape[0] // 2
    top = master_ref[:rows]
    bottom = master_ref[rows:]
    first = pick(low, top, pltpu.roll(top, HALF, 1))
    second = pick(low, pltpu.roll(bottom, HALF, 1), bottom)
    packed = jnp.where(lane_of(top.shape) < HALF, first, second).astype(BF16)
    for owner in range(send_ref.shape[0]):
        send_ref[owner] = packed
    near_ref[:2] = volume_ref[0]
    near_ref[2] = pick(low, cot_ref[0, 0].astype(F32), cot_ref[0, 1].astype(F32)).astype(BF16)
    slab_ref[:2] = volume_ref[0]
    slab_ref[2:] = cot_ref[0]


def shifted(plane, dy, dx):
    _, cols, width = plane.shape
    if dx:
        at = lax.broadcasted_iota(jnp.int32, plane.shape, 1)
        keep = at < cols - 1 if dx > 0 else at > 0
        plane = jnp.where(keep, pltpu.roll(plane, (-dx) % cols, 1), 0.0)
    if dy:
        gap = jnp.zeros((1, cols, width), plane.dtype)
        plane = jnp.concatenate([plane[1:], gap] if dy > 0 else [gap, plane[:-1]], axis=0)
    return plane


def tap_pieces(plane, sign):
    columns = [shifted(plane, 0, sign * (f - 1)) for f in range(3)]
    return [shifted(columns[f], sign * (e - 1), 0) for e in range(3) for f in range(3)]


def kernel_rows(low, mine, other):
    mine = mine.astype(F32)
    other = other.astype(F32)
    left = pick(low, mine, other)
    right = pick(low, other, mine)
    keep = lane_of(left.shape) < HALF
    first = jnp.where(keep, left, pltpu.roll(right, HALF, 1))
    second = jnp.where(keep, pltpu.roll(left, HALF, 1), right)
    return first.astype(BF16), second.astype(BF16)


def forward_body(
    kernel_ref,
    got_ref,
    volume_ref,
    cot_ref,
    near_ref,
    out_act_ref,
    grad_ref,
    weight_ref,
    window_ref,
    wide_ref,
    deep_ref,
    turned_ref,
    stack_ref,
    total_ref,
):
    low = core_is_low()
    owners, rows, width = kernel_ref.shape
    shape = volume_ref.shape[2:]
    cells = shape[0] * shape[1]
    halves = owners * rows

    def handed(index):
        return got_ref[halves + index * cells : halves + (index + 1) * cells].astype(F32).reshape(shape)

    own = [volume_ref[0, i].astype(F32) for i in range(2)]
    near = [near_ref[i].astype(F32) for i in range(3)]
    far = [handed(i) for i in range(3)]
    beside = [handed(3 + i) for i in range(4)]
    planes = [pick(low, near[i], far[i]) for i in range(2)]
    planes += [pick(low, own[i], beside[i]) for i in range(2)]
    planes += [pick(low, beside[i], own[i]) for i in range(2)]
    planes += [pick(low, far[i], near[i]) for i in range(2)]
    for index, plane in enumerate(planes):
        for tap, piece in enumerate(tap_pieces(plane, 1)):
            window_ref[index * cells : (index + 1) * cells, tap * width : (tap + 1) * width] = (
                piece.reshape(cells, width).astype(BF16)
            )
    cot_own = [cot_ref[0, i].astype(F32) for i in range(2)]
    cots = [pick(low, near[2], far[2])]
    cots += [pick(low, cot_own[i], beside[2 + i]) for i in range(2)]
    cots += [pick(low, beside[2 + i], cot_own[i]) for i in range(2)]
    cots += [pick(low, far[2], near[2])]
    cotangent = jnp.concatenate([c.reshape(cells, width) for c in cots], axis=0)
    group = owners // 3
    for owner in range(owners):
        offset, j = divmod(owner, group)
        blocks = kernel_rows(low, kernel_ref[owner], got_ref[owner * rows : (owner + 1) * rows])
        for k in range(2):
            at = slice((2 * j + k) * rows, (2 * j + k + 1) * rows)
            if offset < 2:
                wide_ref[at, offset * width : (offset + 1) * width] = blocks[k]
            else:
                deep_ref[at] = blocks[k]
    count = 6 * cells
    inner = 4 * cells
    span = 9 * width
    product = jnp.dot(window_ref[: count + cells], wide_ref[...], preferred_element_type=F32)
    preact = jnp.dot(window_ref[2 * cells :], deep_ref[...], preferred_element_type=F32)
    preact = preact + product[:count, :width] + product[cells:, width:]
    sigma = jax.nn.sigmoid(preact)
    slope = sigma * (1.0 + preact * (1.0 - sigma))
    act = preact[cells : cells + inner] * sigma[cells : cells + inner]
    act = pick(low, act[: inner // 2], act[inner // 2 :])
    out_act_ref[0] = act.reshape(out_act_ref.shape[1:]).astype(BF16)
    grad = cotangent * slope
    grad_ref[...] = pick(low, grad[:inner], grad[2 * cells :]).astype(BF16)
    turned_ref[...] = grad[cells : cells + inner].T
    mine = pick(low, turned_ref[:HALF], turned_ref[HALF:]).astype(BF16)
    stack_ref[...] = jnp.zeros_like(stack_ref)
    for offset in range(3):
        stack_ref[offset * HALF : (offset + 1) * HALF, offset * cells : offset * cells + inner] = mine
    stacked = jnp.dot(stack_ref[...], window_ref[cells : cells + count], preferred_element_type=F32)
    for offset in range(3):
        total_ref[:, offset * span : (offset + 1) * span] = stacked[offset * HALF : (offset + 1) * HALF]
    lane = lane_of((HALF, width))

    def columns(start):
        tile, offset = divmod(start, width)
        here = total_ref[:, tile * width : (tile + 1) * width]
        if not offset:
            return here
        here = pltpu.roll(here, width - offset, 1)
        if (tile + 1) * width >= total_ref.shape[1]:
            return here
        after = pltpu.roll(total_ref[:, (tile + 1) * width : (tile + 2) * width], width - offset, 1)
        return jnp.where(lane < width - offset, here, after)

    shard = 2 * rows
    rest = shard - 2 * width
    folds = width // rest
    lines = HALF // folds
    for owner in range(owners):
        start = owner * shard
        weight_ref[owner, :HALF] = columns(start).astype(BF16)
        weight_ref[owner, HALF : 2 * HALF] = columns(start + width).astype(BF16)
        tail = columns(start + 2 * width)
        folded = tail[:lines]
        for fold in range(1, folds):
            part = pltpu.roll(tail[fold * lines : (fold + 1) * lines], fold * rest, 1)
            folded = jnp.where(lane[:lines] >= fold * rest, part, folded)
        weight_ref[owner, 2 * HALF :] = folded.astype(BF16)


def backward_body(kernel_ref, got_ref, grad_ref, out_ref, window_ref, turn_ref):
    low = core_is_low()
    owners, rows, width = kernel_ref.shape
    shape = out_ref.shape[2:]
    cells = grad_ref.shape[0] // 4
    for owner in range(owners):
        blocks = kernel_rows(low, kernel_ref[owner], got_ref[owner * rows : (owner + 1) * rows])
        for k in range(2):
            turn_ref[(2 * owner + k) * rows : (2 * owner + k + 1) * rows] = blocks[k]
    for index in range(4):
        plane = grad_ref[index * cells : (index + 1) * cells].astype(F32).reshape(shape)
        for tap, piece in enumerate(tap_pieces(plane, -1)):
            window_ref[index * cells : (index + 1) * cells, tap * width : (tap + 1) * width] = (
                piece.reshape(cells, width).astype(BF16)
            )
    total = jnp.zeros((2 * cells, width), F32)
    for offset in range(3):
        for tap in range(9):
            at = (offset * 9 + tap) * width
            total = total + lax.dot_general(
                window_ref[(2 - offset) * cells : (4 - offset) * cells, tap * width : (tap + 1) * width],
                turn_ref[at : at + width],
                (((1,), (1,)), ((), ())),
                preferred_element_type=F32,
            )
    out_ref[0] = total.reshape(2, *shape).astype(BF16)


def update_body(cells_all, grads_ref, master_ref, moment_ref, second_ref, out_ref, out_m_ref, out_s_ref, grad_ref):
    rows, width = master_ref.shape
    pieces = rows // 2 // PIECE
    halves = []
    for half in range(PAIR):
        halves.append(
            jnp.concatenate([grads_ref[PAIR * i + half] for i in range(pieces)], axis=0)
        )
    rest = rows - 2 * width
    folds = width // rest
    group = HALF // folds
    for part in range(2):
        both = jnp.concatenate([h[part * HALF : (part + 1) * HALF] for h in halves], axis=0)
        grad_ref[part * width : (part + 1) * width] = both.T
    tails = []
    for h in halves:
        tail = h[2 * HALF :]
        for fold in range(folds):
            tails.append(pltpu.roll(tail, width - fold * rest, 1) if fold else tail)
    assert len(tails) * group == width
    grad_ref[2 * width :] = jnp.concatenate(tails, axis=0).T[:rest]
    weight_grad = grad_ref[...] / math.sqrt(cells_all)
    moment_next = 0.9 * moment_ref[...] + 0.1 * weight_grad
    second_next = 0.999 * second_ref[...] + 0.001 * weight_grad * weight_grad
    master = master_ref[...]
    out_ref[...] = master - 0.001 * (moment_next / (jnp.sqrt(second_next) + 1e-08) + 0.01 * master)
    out_m_ref[...] = moment_next
    out_s_ref[...] = second_next


def exchanged(tiles, groups):
    return lax.all_to_all(tiles, "spatial", 0, 0, tiled=True, axis_index_groups=groups)


def moved(value, perm):
    return lax.ppermute(value, "spatial", perm)


def layer(volume, cotangent, master, moment, second):
    _, planes, rows, cols, width = volume.shape
    cells = rows * cols
    owners = lax.axis_size("dp")
    count = lax.axis_size("spatial")
    shard = master.shape[0]
    taps_all = owners * shard
    like = jax.ShapeDtypeStruct

    def inside(pairs):
        return [(i, j) for i, j in pairs if 0 <= j < count]

    swap = [(i, i ^ 1) for i in range(count)]
    outward = inside((i, i - 1 if i % 2 == 0 else i + 1) for i in range(count))

    packed = like((owners, shard // 2, width), BF16)
    send, edge, slab = pl.pallas_call(
        pack_body,
        out_shape=(packed, like((3, rows, cols, width), BF16), like((4, rows, cols, width), BF16)),
        name="pack",
        compiler_params=pltpu.CompilerParams(vmem_limit_bytes=8 << 20),
    )(master, volume, cotangent)
    halves = lax.all_to_all(send, "dp", 0, 0, tiled=True)
    near = moved(edge, outward)
    whole = jnp.concatenate([v.reshape(-1, width) for v in (halves, near, slab)], axis=0)
    got = moved(whole, swap)
    activation, grad, weight = pl.pallas_call(
        forward_body,
        out_shape=(like(volume.shape, BF16), like((4 * cells, width), BF16), packed),
        scratch_shapes=[
            pltpu.VMEM((8 * cells, 9 * width), BF16),
            pltpu.VMEM((9 * width, 2 * width), BF16),
            pltpu.VMEM((9 * width, width), BF16),
            pltpu.VMEM((width, 4 * cells), F32),
            pltpu.VMEM((3 * HALF, 6 * cells), BF16),
            pltpu.VMEM((HALF, taps_all), F32),
        ],
        name="forward",
        compiler_params=pltpu.CompilerParams(vmem_limit_bytes=28 << 20),
    )(halves, got, volume, cotangent, near)
    arrived = lax.all_to_all(weight, "dp", 0, 0, tiled=True)
    input_grad = pl.pallas_call(
        backward_body,
        out_shape=like(volume.shape, BF16),
        scratch_shapes=[
            pltpu.VMEM((4 * cells, 9 * width), BF16),
            pltpu.VMEM((taps_all, width), BF16),
        ],
        cost_estimate=pl.CostEstimate(
            flops=2 * 2 * cells * taps_all * width, bytes_accessed=taps_all * width, transcendentals=0
        ),
        name="backward",
    compiler_params=pltpu.CompilerParams(vmem_limit_bytes=20 << 20),
    )(halves, got, grad)

    same_y = [
        [(y * MIDDLE + h) * PAIR + c for h in range(MIDDLE)] for y in range(OUTER) for c in range(PAIR)
    ]
    same_rest = [[y * MIDDLE * PAIR + r for y in range(OUTER)] for r in range(MIDDLE * PAIR)]
    same_z = [
        [(y * MIDDLE + h) * PAIR + c for y in range(OUTER) for c in range(PAIR)] for h in range(MIDDLE)
    ]
    pieces = shard // 2 // PIECE
    summed = arrived.astype(F32).sum(axis=0).reshape(pieces, PIECE, width)
    summed = jnp.pad(summed, ((0, OUTER - pieces), (0, 0), (0, 0)))
    piece = exchanged(summed, same_rest)
    piece = piece.sum(0)
    piece = exchanged(jnp.broadcast_to(piece[None], (MIDDLE, PIECE, width)), same_y)
    piece = piece.sum(0)
    joined = exchanged(jnp.broadcast_to(piece[None], (OUTER * PAIR, PIECE, width)), same_z)
    cells_all = owners * count * planes * cells
    state = like(master.shape, F32)
    master_next, moment_next, second_next = pl.pallas_call(
        functools.partial(update_body, cells_all),
        out_shape=(state, state, state),
        scratch_shapes=[pltpu.VMEM(master.shape, F32)],
        name="update",
        compiler_params=pltpu.CompilerParams(vmem_limit_bytes=8 << 20),
    )(joined, master, moment, second)
    return (activation, input_grad, master_next, moment_next, second_next)


def solution(mesh):
    return jax.shard_map(
        layer,
        mesh=mesh,
        in_specs=(
            P("dp", "spatial", None, None, None),
            P("dp", "spatial", None, None, None),
            P("dp", None),
            P("dp", None),
            P("dp", None),
        ),
        out_specs=(
            P("dp", "spatial", None, None, None),
            P("dp", "spatial", None, None, None),
            P("dp", None),
            P("dp", None),
            P("dp", None),
        ),
        check_vma=False,
    )
```

```python
import functools
import math

import jax
import jax.numpy as jnp
from jax import lax
from jax.experimental import pallas as pl
from jax.experimental.pallas import tpu as pltpu
from jax.sharding import PartitionSpec as P

F32 = jnp.float32
BF16 = jnp.bfloat16
OUTER = 8
MIDDLE = 4
PAIR = 2
HALF = 64
PIECE = 24


def core_is_low():
    return lax.rem(lax.axis_index("spatial"), PAIR) == 0


def lane_of(shape):
    return lax.broadcasted_iota(jnp.int32, shape, len(shape) - 1)


def pick(low, when_low, when_high):
    return jnp.where(low, when_low, when_high)


def pack_body(master_ref, send_ref):
    low = core_is_low()
    rows = master_ref.shape[0] // 2
    top = master_ref[:rows]
    bottom = master_ref[rows:]
    first = pick(low, top, pltpu.roll(top, HALF, 1))
    second = pick(low, pltpu.roll(bottom, HALF, 1), bottom)
    packed = jnp.where(lane_of(top.shape) < HALF, first, second).astype(BF16)
    for owner in range(send_ref.shape[0]):
        send_ref[owner] = packed


def edges_body(volume_ref, cot_ref, near_ref, slab_ref):
    low = core_is_low()
    near_ref[:2] = volume_ref[0]
    near_ref[2] = pick(low, cot_ref[0, 0].astype(F32), cot_ref[0, 1].astype(F32)).astype(BF16)
    slab_ref[:2] = volume_ref[0]
    slab_ref[2:] = cot_ref[0]


def shifted(plane, dy, dx):
    _, cols, width = plane.shape
    if dx:
        at = lax.broadcasted_iota(jnp.int32, plane.shape, 1)
        keep = at < cols - 1 if dx > 0 else at > 0
        plane = jnp.where(keep, pltpu.roll(plane, (-dx) % cols, 1), 0.0)
    if dy:
        gap = jnp.zeros((1, cols, width), plane.dtype)
        plane = jnp.concatenate([plane[1:], gap] if dy > 0 else [gap, plane[:-1]], axis=0)
    return plane


def tap_pieces(plane, sign):
    columns = [shifted(plane, 0, sign * (f - 1)) for f in range(3)]
    return [shifted(columns[f], sign * (e - 1), 0) for e in range(3) for f in range(3)]


def kernel_rows(low, mine, other):
    mine = mine.astype(F32)
    other = other.astype(F32)
    left = pick(low, mine, other)
    right = pick(low, other, mine)
    keep = lane_of(left.shape) < HALF
    first = jnp.where(keep, left, pltpu.roll(right, HALF, 1))
    second = jnp.where(keep, pltpu.roll(left, HALF, 1), right)
    return first.astype(BF16), second.astype(BF16)


def forward_body(
    kernel_ref,
    got_ref,
    volume_ref,
    cot_ref,
    near_ref,
    out_act_ref,
    grad_ref,
    weight_ref,
    window_ref,
    wide_ref,
    deep_ref,
    turned_ref,
    stack_ref,
    total_ref,
):
    low = core_is_low()
    owners, rows, width = kernel_ref.shape
    shape = volume_ref.shape[2:]
    cells = shape[0] * shape[1]
    halves = owners * rows

    def handed(index):
        return got_ref[halves + index * cells : halves + (index + 1) * cells].astype(F32).reshape(shape)

    own = [volume_ref[0, i].astype(F32) for i in range(2)]
    near = [near_ref[i].astype(F32) for i in range(3)]
    far = [handed(i) for i in range(3)]
    beside = [handed(3 + i) for i in range(4)]
    low_planes = [*near[:2], *own, *beside[:2], far[0]]
    high_planes = [far[1], *beside[:2], *own, *near[:2]]
    planes = [pick(low, x, y) for x, y in zip(low_planes, high_planes)]
    for index, plane in enumerate(planes):
        for tap, piece in enumerate(tap_pieces(plane, 1)):
            window_ref[index * cells : (index + 1) * cells, tap * width : (tap + 1) * width] = (
                piece.reshape(cells, width).astype(BF16)
            )
    cot_own = [cot_ref[0, i].astype(F32) for i in range(2)]
    cots = [pick(low, x, y) for x, y in zip([near[2], *cot_own, *beside[2:]], [*beside[2:], *cot_own, near[2]])]
    cotangent = jnp.concatenate([c.reshape(cells, width) for c in cots], axis=0)
    group = owners // 3
    for owner in range(owners):
        offset, j = divmod(owner, group)
        blocks = kernel_rows(low, kernel_ref[owner], got_ref[owner * rows : (owner + 1) * rows])
        for k in range(2):
            at = slice((2 * j + k) * rows, (2 * j + k + 1) * rows)
            if offset < 2:
                wide_ref[at, offset * width : (offset + 1) * width] = blocks[k]
            else:
                deep_ref[at] = blocks[k]
    count = 5 * cells
    inner = 4 * cells
    span = 9 * width
    product = jnp.dot(window_ref[: count + cells], wide_ref[...], preferred_element_type=F32)
    preact = jnp.dot(window_ref[2 * cells :], deep_ref[...], preferred_element_type=F32)
    preact = preact + product[:count, :width] + product[cells:, width:]
    sigma = jax.nn.sigmoid(preact)
    slope = sigma * (1.0 + preact * (1.0 - sigma))
    act = (preact * sigma)[cells : 4 * cells]
    act = pick(low, act[: inner // 2], act[cells:])
    out_act_ref[0] = act.reshape(out_act_ref.shape[1:]).astype(BF16)
    grad = cotangent * slope
    grad_ref[...] = pick(low, grad[:inner], grad[cells:]).astype(BF16)
    turned_ref[...] = pick(low, grad[cells:], grad[:inner]).T
    mine = pick(low, turned_ref[:HALF], turned_ref[HALF:]).astype(BF16)
    stack_ref[...] = jnp.zeros_like(stack_ref)
    for offset in range(3):
        stack_ref[offset * HALF : (offset + 1) * HALF, offset * cells : offset * cells + inner] = mine
    at = pl.multiple_of(jnp.where(low, cells, 0), cells)
    stacked = jnp.dot(stack_ref[...], window_ref[pl.ds(at, 6 * cells)], preferred_element_type=F32)
    for offset in range(3):
        total_ref[:, offset * span : (offset + 1) * span] = stacked[offset * HALF : (offset + 1) * HALF]
    lane = lane_of((HALF, width))

    def columns(start):
        tile, offset = divmod(start, width)
        here = total_ref[:, tile * width : (tile + 1) * width]
        if not offset:
            return here
        here = pltpu.roll(here, width - offset, 1)
        if (tile + 1) * width >= total_ref.shape[1]:
            return here
        after = pltpu.roll(total_ref[:, (tile + 1) * width : (tile + 2) * width], width - offset, 1)
        return jnp.where(lane < width - offset, here, after)

    shard = 2 * rows
    rest = shard - 2 * width
    folds = width // rest
    lines = HALF // folds
    for owner in range(owners):
        start = owner * shard
        weight_ref[owner, :HALF] = columns(start).astype(BF16)
        weight_ref[owner, HALF : 2 * HALF] = columns(start + width).astype(BF16)
        tail = columns(start + 2 * width)
        folded = tail[:lines]
        for fold in range(1, folds):
            part = pltpu.roll(tail[fold * lines : (fold + 1) * lines], fold * rest, 1)
            folded = jnp.where(lane[:lines] >= fold * rest, part, folded)
        weight_ref[owner, 2 * HALF :] = folded.astype(BF16)


def backward_body(kernel_ref, got_ref, grad_ref, out_ref, window_ref, turn_ref):
    low = core_is_low()
    owners, rows, width = kernel_ref.shape
    shape = out_ref.shape[2:]
    cells = grad_ref.shape[0] // 4
    for owner in range(owners):
        blocks = kernel_rows(low, kernel_ref[owner], got_ref[owner * rows : (owner + 1) * rows])
        for k in range(2):
            turn_ref[(2 * owner + k) * rows : (2 * owner + k + 1) * rows] = blocks[k]
    for index in range(4):
        plane = grad_ref[index * cells : (index + 1) * cells].astype(F32).reshape(shape)
        for tap, piece in enumerate(tap_pieces(plane, -1)):
            window_ref[index * cells : (index + 1) * cells, tap * width : (tap + 1) * width] = (
                piece.reshape(cells, width).astype(BF16)
            )
    total = jnp.zeros((2 * cells, width), F32)
    for offset in range(3):
        for tap in range(9):
            at = (offset * 9 + tap) * width
            total = total + lax.dot_general(
                window_ref[(2 - offset) * cells : (4 - offset) * cells, tap * width : (tap + 1) * width],
                turn_ref[at : at + width],
                (((1,), (1,)), ((), ())),
                preferred_element_type=F32,
            )
    out_ref[0] = total.reshape(2, *shape).astype(BF16)


def update_body(cells_all, grads_ref, master_ref, moment_ref, second_ref, out_ref, out_m_ref, out_s_ref, grad_ref):
    rows, width = master_ref.shape
    pieces = rows // 2 // PIECE
    halves = []
    for half in range(PAIR):
        halves.append(
            jnp.concatenate([grads_ref[PAIR * i + half] for i in range(pieces)], axis=0)
        )
    rest = rows - 2 * width
    folds = width // rest
    group = HALF // folds
    for part in range(2):
        both = jnp.concatenate([h[part * HALF : (part + 1) * HALF] for h in halves], axis=0)
        grad_ref[part * width : (part + 1) * width] = both.T
    tails = []
    for h in halves:
        tail = h[2 * HALF :]
        for fold in range(folds):
            tails.append(pltpu.roll(tail, width - fold * rest, 1) if fold else tail)
    assert len(tails) * group == width
    grad_ref[2 * width :] = jnp.concatenate(tails, axis=0).T[:rest]
    weight_grad = grad_ref[...] / math.sqrt(cells_all)
    moment_next = 0.9 * moment_ref[...] + 0.1 * weight_grad
    second_next = 0.999 * second_ref[...] + 0.001 * weight_grad * weight_grad
    master = master_ref[...]
    out_ref[...] = master - 0.001 * (moment_next / (jnp.sqrt(second_next) + 1e-08) + 0.01 * master)
    out_m_ref[...] = moment_next
    out_s_ref[...] = second_next


def exchanged(tiles, groups):
    return lax.all_to_all(tiles, "spatial", 0, 0, tiled=True, axis_index_groups=groups)


def moved(value, perm):
    return lax.ppermute(value, "spatial", perm)


def layer(volume, cotangent, master, moment, second):
    _, planes, rows, cols, width = volume.shape
    cells = rows * cols
    owners = lax.axis_size("dp")
    count = lax.axis_size("spatial")
    shard = master.shape[0]
    taps_all = owners * shard
    like = jax.ShapeDtypeStruct

    def inside(pairs):
        return [(i, j) for i, j in pairs if 0 <= j < count]

    swap = [(i, i ^ 1) for i in range(count)]
    outward = inside((i, i - 1 if i % 2 == 0 else i + 1) for i in range(count))

    packed = like((owners, shard // 2, width), BF16)
    send = pl.pallas_call(
        pack_body,
        out_shape=packed,
        name="pack",
        compiler_params=pltpu.CompilerParams(vmem_limit_bytes=8 << 20),
    )(master)
    halves = lax.all_to_all(send, "dp", 0, 0, tiled=True)
    edge, slab = pl.pallas_call(
        edges_body,
        out_shape=(like((3, rows, cols, width), BF16), like((4, rows, cols, width), BF16)),
        name="edges",
        compiler_params=pltpu.CompilerParams(vmem_limit_bytes=4 << 20),
    )(volume, cotangent)
    near = moved(edge, outward)
    whole = jnp.concatenate([v.reshape(-1, width) for v in (halves, near, slab)], axis=0)
    got = moved(whole, swap)
    activation, grad, weight = pl.pallas_call(
        forward_body,
        out_shape=(like(volume.shape, BF16), like((4 * cells, width), BF16), packed),
        scratch_shapes=[
            pltpu.VMEM((7 * cells, 9 * width), BF16),
            pltpu.VMEM((9 * width, 2 * width), BF16),
            pltpu.VMEM((9 * width, width), BF16),
            pltpu.VMEM((width, 4 * cells), F32),
            pltpu.VMEM((3 * HALF, 6 * cells), BF16),
            pltpu.VMEM((HALF, taps_all), F32),
        ],
        name="forward",
        compiler_params=pltpu.CompilerParams(vmem_limit_bytes=28 << 20),
    )(halves, got, volume, cotangent, near)
    arrived = lax.all_to_all(weight, "dp", 0, 0, tiled=True)
    input_grad = pl.pallas_call(
        backward_body,
        out_shape=like(volume.shape, BF16),
        scratch_shapes=[
            pltpu.VMEM((4 * cells, 9 * width), BF16),
            pltpu.VMEM((taps_all, width), BF16),
        ],
        cost_estimate=pl.CostEstimate(
            flops=2 * 2 * cells * taps_all * width, bytes_accessed=taps_all * width, transcendentals=0
        ),
        name="backward",
    compiler_params=pltpu.CompilerParams(vmem_limit_bytes=20 << 20),
    )(halves, got, grad)

    same_y = [
        [(y * MIDDLE + h) * PAIR + c for h in range(MIDDLE)] for y in range(OUTER) for c in range(PAIR)
    ]
    same_rest = [[y * MIDDLE * PAIR + r for y in range(OUTER)] for r in range(MIDDLE * PAIR)]
    same_z = [
        [(y * MIDDLE + h) * PAIR + c for y in range(OUTER) for c in range(PAIR)] for h in range(MIDDLE)
    ]
    pieces = shard // 2 // PIECE
    summed = arrived.astype(F32).sum(axis=0).reshape(pieces, PIECE, width)
    summed = jnp.pad(summed, ((0, OUTER - pieces), (0, 0), (0, 0)))
    piece = exchanged(summed, same_rest)
    piece = piece.sum(0)
    piece = exchanged(jnp.broadcast_to(piece[None], (MIDDLE, PIECE, width)), same_y)
    piece = piece.sum(0)
    joined = exchanged(jnp.broadcast_to(piece[None], (OUTER * PAIR, PIECE, width)), same_z)
    cells_all = owners * count * planes * cells
    state = like(master.shape, F32)
    master_next, moment_next, second_next = pl.pallas_call(
        functools.partial(update_body, cells_all),
        out_shape=(state, state, state),
        scratch_shapes=[pltpu.VMEM(master.shape, F32)],
        name="update",
        compiler_params=pltpu.CompilerParams(vmem_limit_bytes=8 << 20),
    )(joined, master, moment, second)
    return (activation, input_grad, master_next, moment_next, second_next)


def solution(mesh):
    return jax.shard_map(
        layer,
        mesh=mesh,
        in_specs=(
            P("dp", "spatial", None, None, None),
            P("dp", "spatial", None, None, None),
            P("dp", None),
            P("dp", None),
            P("dp", None),
        ),
        out_specs=(
            P("dp", "spatial", None, None, None),
            P("dp", "spatial", None, None, None),
            P("dp", None),
            P("dp", None),
            P("dp", None),
        ),
        check_vma=False,
    )
```

```python
import functools
import math

import jax
import jax.numpy as jnp
from jax import lax
from jax.experimental import pallas as pl
from jax.experimental.pallas import tpu as pltpu
from jax.sharding import PartitionSpec as P

F32 = jnp.float32
BF16 = jnp.bfloat16
OUTER = 8
MIDDLE = 4
PAIR = 2
HALF = 64
PIECE = 24


def core_is_low():
    return lax.rem(lax.axis_index("spatial"), PAIR) == 0


def lane_of(shape):
    return lax.broadcasted_iota(jnp.int32, shape, len(shape) - 1)


def pick(low, when_low, when_high):
    return jnp.where(low, when_low, when_high)


def pack_body(master_ref, send_ref):
    low = core_is_low()
    rows = master_ref.shape[0] // 2
    top = master_ref[:rows]
    bottom = master_ref[rows:]
    first = pick(low, top, pltpu.roll(top, HALF, 1))
    second = pick(low, pltpu.roll(bottom, HALF, 1), bottom)
    packed = jnp.where(lane_of(top.shape) < HALF, first, second).astype(BF16)
    for owner in range(send_ref.shape[0]):
        send_ref[owner] = packed


def edges_body(volume_ref, cot_ref, near_ref, slab_ref):
    low = core_is_low()
    near_ref[:2] = volume_ref[0]
    near_ref[2] = pick(low, cot_ref[0, 0].astype(F32), cot_ref[0, 1].astype(F32)).astype(BF16)
    slab_ref[:2] = volume_ref[0]
    slab_ref[2:] = cot_ref[0]


def shifted(plane, dy, dx):
    _, cols, width = plane.shape
    if dx:
        at = lax.broadcasted_iota(jnp.int32, plane.shape, 1)
        keep = at < cols - 1 if dx > 0 else at > 0
        plane = jnp.where(keep, pltpu.roll(plane, (-dx) % cols, 1), 0.0)
    if dy:
        gap = jnp.zeros((1, cols, width), plane.dtype)
        plane = jnp.concatenate([plane[1:], gap] if dy > 0 else [gap, plane[:-1]], axis=0)
    return plane


def tap_pieces(plane, sign):
    columns = [shifted(plane, 0, sign * (f - 1)) for f in range(3)]
    return [shifted(columns[f], sign * (e - 1), 0) for e in range(3) for f in range(3)]


def kernel_rows(low, mine, other):
    mine = mine.astype(F32)
    other = other.astype(F32)
    left = pick(low, mine, other)
    right = pick(low, other, mine)
    keep = lane_of(left.shape) < HALF
    first = jnp.where(keep, left, pltpu.roll(right, HALF, 1))
    second = jnp.where(keep, pltpu.roll(left, HALF, 1), right)
    return first.astype(BF16), second.astype(BF16)


def forward_body(
    kernel_ref,
    got_ref,
    volume_ref,
    cot_ref,
    near_ref,
    out_act_ref,
    grad_ref,
    weight_ref,
    window_ref,
    wide_ref,
    deep_ref,
    turned_ref,
    stack_ref,
    total_ref,
):
    low = core_is_low()
    owners, rows, width = kernel_ref.shape
    shape = volume_ref.shape[2:]
    cells = shape[0] * shape[1]
    halves = owners * rows

    def handed(index):
        return got_ref[halves + index * cells : halves + (index + 1) * cells].astype(F32).reshape(shape)

    own = [volume_ref[0, i].astype(F32) for i in range(2)]
    near = [near_ref[i].astype(F32) for i in range(3)]
    far = [handed(i) for i in range(3)]
    beside = [handed(3 + i) for i in range(4)]
    low_planes = [*near[:2], *own, *beside[:2], far[0]]
    high_planes = [far[1], *beside[:2], *own, *near[:2]]
    planes = [pick(low, x, y) for x, y in zip(low_planes, high_planes)]
    for index, plane in enumerate(planes):
        for tap, piece in enumerate(tap_pieces(plane, 1)):
            window_ref[index * cells : (index + 1) * cells, tap * width : (tap + 1) * width] = (
                piece.reshape(cells, width).astype(BF16)
            )
    cot_own = [cot_ref[0, i].astype(F32) for i in range(2)]
    cots = [pick(low, x, y) for x, y in zip([near[2], *cot_own, *beside[2:]], [*beside[2:], *cot_own, near[2]])]
    cotangent = jnp.concatenate([c.reshape(cells, width) for c in cots], axis=0)
    group = owners // 3
    for owner in range(owners):
        offset, j = divmod(owner, group)
        blocks = kernel_rows(low, kernel_ref[owner], got_ref[owner * rows : (owner + 1) * rows])
        for k in range(2):
            at = slice((2 * j + k) * rows, (2 * j + k + 1) * rows)
            if offset < 2:
                wide_ref[at, offset * width : (offset + 1) * width] = blocks[k]
            else:
                deep_ref[at] = blocks[k]
    count = 5 * cells
    inner = 4 * cells
    span = 9 * width
    product = jnp.dot(window_ref[: count + cells], wide_ref[...], preferred_element_type=F32)
    part = count // 2
    preact = jnp.concatenate(
        [
            jnp.dot(
                window_ref[2 * cells + i * part : 2 * cells + (i + 1) * part],
                deep_ref[...],
                preferred_element_type=F32,
            )
            for i in range(2)
        ],
        axis=0,
    )
    preact = preact + product[:count, :width] + product[cells:, width:]
    sigma = jax.nn.sigmoid(preact)
    slope = sigma * (1.0 + preact * (1.0 - sigma))
    act = (preact * sigma)[cells : 4 * cells]
    act = pick(low, act[: inner // 2], act[cells:])
    out_act_ref[0] = act.reshape(out_act_ref.shape[1:]).astype(BF16)
    grad = cotangent * slope
    grad_ref[...] = pick(low, grad[:inner], grad[cells:]).astype(BF16)
    turned_ref[...] = pick(low, grad[cells:], grad[:inner]).T
    mine = pick(low, turned_ref[:HALF], turned_ref[HALF:]).astype(BF16)
    stack_ref[...] = jnp.zeros_like(stack_ref)
    for offset in range(3):
        stack_ref[offset * HALF : (offset + 1) * HALF, offset * cells : offset * cells + inner] = mine
    at = pl.multiple_of(jnp.where(low, cells, 0), cells)
    for left, right in ((0, 5 * width), (5 * width, span)):
        stacked = jnp.dot(
            stack_ref[...], window_ref[pl.ds(at, 6 * cells), left:right], preferred_element_type=F32
        )
        for offset in range(3):
            total_ref[:, offset * span + left : offset * span + right] = stacked[
                offset * HALF : (offset + 1) * HALF
            ]
    lane = lane_of((HALF, width))

    def columns(start):
        tile, offset = divmod(start, width)
        here = total_ref[:, tile * width : (tile + 1) * width]
        if not offset:
            return here
        here = pltpu.roll(here, width - offset, 1)
        if (tile + 1) * width >= total_ref.shape[1]:
            return here
        after = pltpu.roll(total_ref[:, (tile + 1) * width : (tile + 2) * width], width - offset, 1)
        return jnp.where(lane < width - offset, here, after)

    shard = 2 * rows
    rest = shard - 2 * width
    folds = width // rest
    lines = HALF // folds
    for owner in range(owners):
        start = owner * shard
        weight_ref[owner, :HALF] = columns(start).astype(BF16)
        weight_ref[owner, HALF : 2 * HALF] = columns(start + width).astype(BF16)
        tail = columns(start + 2 * width)
        folded = tail[:lines]
        for fold in range(1, folds):
            part = pltpu.roll(tail[fold * lines : (fold + 1) * lines], fold * rest, 1)
            folded = jnp.where(lane[:lines] >= fold * rest, part, folded)
        weight_ref[owner, 2 * HALF :] = folded.astype(BF16)


def backward_body(kernel_ref, got_ref, grad_ref, out_ref, window_ref, turn_ref):
    low = core_is_low()
    owners, rows, width = kernel_ref.shape
    shape = out_ref.shape[2:]
    cells = grad_ref.shape[0] // 4
    for owner in range(owners):
        blocks = kernel_rows(low, kernel_ref[owner], got_ref[owner * rows : (owner + 1) * rows])
        for k in range(2):
            turn_ref[(2 * owner + k) * rows : (2 * owner + k + 1) * rows] = blocks[k]
    for index in range(4):
        plane = grad_ref[index * cells : (index + 1) * cells].astype(F32).reshape(shape)
        for tap, piece in enumerate(tap_pieces(plane, -1)):
            window_ref[index * cells : (index + 1) * cells, tap * width : (tap + 1) * width] = (
                piece.reshape(cells, width).astype(BF16)
            )
    total = jnp.zeros((2 * cells, width), F32)
    for offset in range(3):
        for tap in range(9):
            at = (offset * 9 + tap) * width
            total = total + lax.dot_general(
                window_ref[(2 - offset) * cells : (4 - offset) * cells, tap * width : (tap + 1) * width],
                turn_ref[at : at + width],
                (((1,), (1,)), ((), ())),
                preferred_element_type=F32,
            )
    out_ref[0] = total.reshape(2, *shape).astype(BF16)


def finish_body(
    cells_all,
    grads_ref,
    master_ref,
    moment_ref,
    second_ref,
    kernel_ref,
    got_ref,
    hidden_ref,
    out_ref,
    out_m_ref,
    out_s_ref,
    out_input_ref,
    grad_ref,
    window_ref,
    turn_ref,
):
    update_body(cells_all, grads_ref, master_ref, moment_ref, second_ref, out_ref, out_m_ref, out_s_ref, grad_ref)
    backward_body(kernel_ref, got_ref, hidden_ref, out_input_ref, window_ref, turn_ref)


def update_body(cells_all, grads_ref, master_ref, moment_ref, second_ref, out_ref, out_m_ref, out_s_ref, grad_ref):
    rows, width = master_ref.shape
    pieces = rows // 2 // PIECE
    halves = []
    for half in range(PAIR):
        halves.append(
            jnp.concatenate([grads_ref[PAIR * i + half] for i in range(pieces)], axis=0)
        )
    rest = rows - 2 * width
    folds = width // rest
    group = HALF // folds
    for part in range(2):
        both = jnp.concatenate([h[part * HALF : (part + 1) * HALF] for h in halves], axis=0)
        grad_ref[part * width : (part + 1) * width] = both.T
    tails = []
    for h in halves:
        tail = h[2 * HALF :]
        for fold in range(folds):
            tails.append(pltpu.roll(tail, width - fold * rest, 1) if fold else tail)
    assert len(tails) * group == width
    grad_ref[2 * width :] = jnp.concatenate(tails, axis=0).T[:rest]
    weight_grad = grad_ref[...] / math.sqrt(cells_all)
    moment_next = 0.9 * moment_ref[...] + 0.1 * weight_grad
    second_next = 0.999 * second_ref[...] + 0.001 * weight_grad * weight_grad
    master = master_ref[...]
    out_ref[...] = master - 0.001 * (moment_next / (jnp.sqrt(second_next) + 1e-08) + 0.01 * master)
    out_m_ref[...] = moment_next
    out_s_ref[...] = second_next


def exchanged(tiles, groups):
    return lax.all_to_all(tiles, "spatial", 0, 0, tiled=True, axis_index_groups=groups)


def moved(value, perm):
    return lax.ppermute(value, "spatial", perm)


def layer(volume, cotangent, master, moment, second):
    _, planes, rows, cols, width = volume.shape
    cells = rows * cols
    owners = lax.axis_size("dp")
    count = lax.axis_size("spatial")
    shard = master.shape[0]
    taps_all = owners * shard
    like = jax.ShapeDtypeStruct

    def inside(pairs):
        return [(i, j) for i, j in pairs if 0 <= j < count]

    swap = [(i, i ^ 1) for i in range(count)]
    outward = inside((i, i - 1 if i % 2 == 0 else i + 1) for i in range(count))

    packed = like((owners, shard // 2, width), BF16)
    send = pl.pallas_call(
        pack_body,
        out_shape=packed,
        name="pack",
        compiler_params=pltpu.CompilerParams(vmem_limit_bytes=8 << 20),
    )(master)
    halves = lax.all_to_all(send, "dp", 0, 0, tiled=True)
    edge, slab = pl.pallas_call(
        edges_body,
        out_shape=(like((3, rows, cols, width), BF16), like((4, rows, cols, width), BF16)),
        name="edges",
        compiler_params=pltpu.CompilerParams(vmem_limit_bytes=4 << 20),
    )(volume, cotangent)
    near = moved(edge, outward)
    whole = jnp.concatenate([v.reshape(-1, width) for v in (halves, near, slab)], axis=0)
    got = moved(whole, swap)
    activation, grad, weight = pl.pallas_call(
        forward_body,
        out_shape=(like(volume.shape, BF16), like((4 * cells, width), BF16), packed),
        scratch_shapes=[
            pltpu.VMEM((7 * cells, 9 * width), BF16),
            pltpu.VMEM((9 * width, 2 * width), BF16),
            pltpu.VMEM((9 * width, width), BF16),
            pltpu.VMEM((width, 4 * cells), F32),
            pltpu.VMEM((3 * HALF, 6 * cells), BF16),
            pltpu.VMEM((HALF, taps_all), F32),
        ],
        name="forward",
        compiler_params=pltpu.CompilerParams(vmem_limit_bytes=28 << 20),
    )(halves, got, volume, cotangent, near)
    arrived = lax.all_to_all(weight, "dp", 0, 0, tiled=True)
    same_y = [
        [(y * MIDDLE + h) * PAIR + c for h in range(MIDDLE)] for y in range(OUTER) for c in range(PAIR)
    ]
    same_rest = [[y * MIDDLE * PAIR + r for y in range(OUTER)] for r in range(MIDDLE * PAIR)]
    same_z = [
        [(y * MIDDLE + h) * PAIR + c for y in range(OUTER) for c in range(PAIR)] for h in range(MIDDLE)
    ]
    pieces = shard // 2 // PIECE
    summed = arrived.astype(F32).sum(axis=0).reshape(pieces, PIECE, width)
    summed = jnp.pad(summed, ((0, OUTER - pieces), (0, 0), (0, 0)))
    piece = exchanged(summed, same_rest)
    piece = piece.sum(0)
    piece = exchanged(jnp.broadcast_to(piece[None], (MIDDLE, PIECE, width)), same_y)
    piece = piece.sum(0)
    joined = exchanged(jnp.broadcast_to(piece[None], (OUTER * PAIR, PIECE, width)), same_z)
    cells_all = owners * count * planes * cells
    state = like(master.shape, F32)
    master_next, moment_next, second_next, input_grad = pl.pallas_call(
        functools.partial(finish_body, cells_all),
        out_shape=(state, state, state, like(volume.shape, BF16)),
        scratch_shapes=[
            pltpu.VMEM(master.shape, F32),
            pltpu.VMEM((4 * cells, 9 * width), BF16),
            pltpu.VMEM((taps_all, width), BF16),
        ],
        name="finish",
        compiler_params=pltpu.CompilerParams(vmem_limit_bytes=20 << 20),
    )(joined, master, moment, second, halves, got, grad)
    return (activation, input_grad, master_next, moment_next, second_next)


def solution(mesh):
    return jax.shard_map(
        layer,
        mesh=mesh,
        in_specs=(
            P("dp", "spatial", None, None, None),
            P("dp", "spatial", None, None, None),
            P("dp", None),
            P("dp", None),
            P("dp", None),
        ),
        out_specs=(
            P("dp", "spatial", None, None, None),
            P("dp", "spatial", None, None, None),
            P("dp", None),
            P("dp", None),
            P("dp", None),
        ),
        check_vma=False,
    )
```

```python
import functools
import math

import jax
import jax.numpy as jnp
from jax import lax
from jax.experimental import pallas as pl
from jax.experimental.pallas import tpu as pltpu
from jax.sharding import PartitionSpec as P

F32 = jnp.float32
BF16 = jnp.bfloat16
OUTER = 8
MIDDLE = 4
PAIR = 2
HALF = 64
PIECE = 24


def core_is_low():
    return lax.rem(lax.axis_index("spatial"), PAIR) == 0


def lane_of(shape):
    return lax.broadcasted_iota(jnp.int32, shape, len(shape) - 1)


def pick(low, when_low, when_high):
    return jnp.where(low, when_low, when_high)


def pack_body(master_ref, send_ref):
    low = core_is_low()
    rows = master_ref.shape[0] // 2
    top = master_ref[:rows]
    bottom = master_ref[rows:]
    first = pick(low, top, pltpu.roll(top, HALF, 1))
    second = pick(low, pltpu.roll(bottom, HALF, 1), bottom)
    packed = jnp.where(lane_of(top.shape) < HALF, first, second).astype(BF16)
    for owner in range(send_ref.shape[0]):
        send_ref[owner] = packed


def edges_body(volume_ref, cot_ref, near_ref, slab_ref):
    low = core_is_low()
    near_ref[:2] = volume_ref[0]
    near_ref[2] = pick(low, cot_ref[0, 0].astype(F32), cot_ref[0, 1].astype(F32)).astype(BF16)
    slab_ref[:2] = volume_ref[0]
    slab_ref[2:] = cot_ref[0]


def shifted(plane, dy, dx):
    _, cols, width = plane.shape
    if dx:
        at = lax.broadcasted_iota(jnp.int32, plane.shape, 1)
        keep = at < cols - 1 if dx > 0 else at > 0
        plane = jnp.where(keep, pltpu.roll(plane, (-dx) % cols, 1), 0.0)
    if dy:
        gap = jnp.zeros((1, cols, width), plane.dtype)
        plane = jnp.concatenate([plane[1:], gap] if dy > 0 else [gap, plane[:-1]], axis=0)
    return plane


def tap_pieces(plane, sign):
    columns = [shifted(plane, 0, sign * (f - 1)) for f in range(3)]
    return [shifted(columns[f], sign * (e - 1), 0) for e in range(3) for f in range(3)]


def kernel_rows(low, mine, other):
    mine = mine.astype(F32)
    other = other.astype(F32)
    left = pick(low, mine, other)
    right = pick(low, other, mine)
    keep = lane_of(left.shape) < HALF
    first = jnp.where(keep, left, pltpu.roll(right, HALF, 1))
    second = jnp.where(keep, pltpu.roll(left, HALF, 1), right)
    return first.astype(BF16), second.astype(BF16)


def forward_body(
    kernel_ref,
    got_ref,
    volume_ref,
    cot_ref,
    near_ref,
    out_act_ref,
    grad_ref,
    weight_ref,
    window_ref,
    wide_ref,
    deep_ref,
    turned_ref,
    stack_ref,
    total_ref,
):
    low = core_is_low()
    owners, rows, width = kernel_ref.shape
    shape = volume_ref.shape[2:]
    cells = shape[0] * shape[1]
    halves = owners * rows

    def handed(index):
        return got_ref[halves + index * cells : halves + (index + 1) * cells].astype(F32).reshape(shape)

    own = [volume_ref[0, i].astype(F32) for i in range(2)]
    near = [near_ref[i].astype(F32) for i in range(3)]
    far = [handed(i) for i in range(3)]
    beside = [handed(3 + i) for i in range(4)]
    low_planes = [*near[:2], *own, *beside[:2], far[0]]
    high_planes = [far[1], *beside[:2], *own, *near[:2]]
    planes = [pick(low, x, y) for x, y in zip(low_planes, high_planes)]
    for index, plane in enumerate(planes):
        for tap, piece in enumerate(tap_pieces(plane, 1)):
            window_ref[index * cells : (index + 1) * cells, tap * width : (tap + 1) * width] = (
                piece.reshape(cells, width).astype(BF16)
            )
    cot_own = [cot_ref[0, i].astype(F32) for i in range(2)]
    cots = [pick(low, x, y) for x, y in zip([near[2], *cot_own, *beside[2:]], [*beside[2:], *cot_own, near[2]])]
    cotangent = jnp.concatenate([c.reshape(cells, width) for c in cots], axis=0)
    group = owners // 3
    for owner in range(owners):
        offset, j = divmod(owner, group)
        blocks = kernel_rows(low, kernel_ref[owner], got_ref[owner * rows : (owner + 1) * rows])
        for k in range(2):
            at = slice((2 * j + k) * rows, (2 * j + k + 1) * rows)
            if offset < 2:
                wide_ref[at, offset * width : (offset + 1) * width] = blocks[k]
            else:
                deep_ref[at] = blocks[k]
    count = 5 * cells
    inner = 4 * cells
    span = 9 * width
    product = jnp.dot(window_ref[: count + cells], wide_ref[...], preferred_element_type=F32)
    part = count // 2
    preact = jnp.concatenate(
        [
            jnp.dot(
                window_ref[2 * cells + i * part : 2 * cells + (i + 1) * part],
                deep_ref[...],
                preferred_element_type=F32,
            )
            for i in range(2)
        ],
        axis=0,
    )
    preact = preact + product[:count, :width] + product[cells:, width:]
    sigma = jax.nn.sigmoid(preact)
    slope = sigma * (1.0 + preact * (1.0 - sigma))
    act = (preact * sigma)[cells : 4 * cells]
    act = pick(low, act[: inner // 2], act[cells:])
    out_act_ref[0] = act.reshape(out_act_ref.shape[1:]).astype(BF16)
    grad = cotangent * slope
    grad_ref[...] = pick(low, grad[:inner], grad[cells:]).astype(BF16)
    turned_ref[...] = pick(low, grad[cells:], grad[:inner]).T
    mine = pick(low, turned_ref[:HALF], turned_ref[HALF:]).astype(BF16)
    stack_ref[...] = jnp.zeros_like(stack_ref)
    for offset in range(3):
        stack_ref[offset * HALF : (offset + 1) * HALF, offset * cells : offset * cells + inner] = mine
    at = pl.multiple_of(jnp.where(low, cells, 0), cells)
    for left, right in ((0, 5 * width), (5 * width, span)):
        stacked = jnp.dot(
            stack_ref[...], window_ref[pl.ds(at, 6 * cells), left:right], preferred_element_type=F32
        )
        for offset in range(3):
            total_ref[:, offset * span + left : offset * span + right] = stacked[
                offset * HALF : (offset + 1) * HALF
            ]
    lane = lane_of((HALF, width))

    def columns(start):
        tile, offset = divmod(start, width)
        here = total_ref[:, tile * width : (tile + 1) * width]
        if not offset:
            return here
        here = pltpu.roll(here, width - offset, 1)
        if (tile + 1) * width >= total_ref.shape[1]:
            return here
        after = pltpu.roll(total_ref[:, (tile + 1) * width : (tile + 2) * width], width - offset, 1)
        return jnp.where(lane < width - offset, here, after)

    shard = 2 * rows
    rest = shard - 2 * width
    folds = width // rest
    lines = HALF // folds
    for owner in range(owners):
        start = owner * shard
        weight_ref[owner, :HALF] = columns(start).astype(BF16)
        weight_ref[owner, HALF : 2 * HALF] = columns(start + width).astype(BF16)
        tail = columns(start + 2 * width)
        folded = tail[:lines]
        for fold in range(1, folds):
            part = pltpu.roll(tail[fold * lines : (fold + 1) * lines], fold * rest, 1)
            folded = jnp.where(lane[:lines] >= fold * rest, part, folded)
        weight_ref[owner, 2 * HALF :] = folded.astype(BF16)


def backward_body(kernel_ref, got_ref, grad_ref, out_ref, window_ref, turn_ref):
    low = core_is_low()
    owners, rows, width = kernel_ref.shape
    shape = out_ref.shape[2:]
    cells = grad_ref.shape[0] // 4
    for owner in range(owners):
        blocks = kernel_rows(low, kernel_ref[owner], got_ref[owner * rows : (owner + 1) * rows])
        for k in range(2):
            turn_ref[(2 * owner + k) * rows : (2 * owner + k + 1) * rows] = blocks[k]
    for index in range(4):
        plane = grad_ref[index * cells : (index + 1) * cells].astype(F32).reshape(shape)
        for tap, piece in enumerate(tap_pieces(plane, -1)):
            window_ref[index * cells : (index + 1) * cells, tap * width : (tap + 1) * width] = (
                piece.reshape(cells, width).astype(BF16)
            )
    total = jnp.zeros((2 * cells, width), F32)
    for offset in range(3):
        for tap in range(9):
            at = (offset * 9 + tap) * width
            total = total + lax.dot_general(
                window_ref[(2 - offset) * cells : (4 - offset) * cells, tap * width : (tap + 1) * width],
                turn_ref[at : at + width],
                (((1,), (1,)), ((), ())),
                preferred_element_type=F32,
            )
    out_ref[0] = total.reshape(2, *shape).astype(BF16)


def update_body(cells_all, grads_ref, master_ref, moment_ref, second_ref, out_ref, out_m_ref, out_s_ref, grad_ref):
    rows, width = master_ref.shape
    pieces = rows // 2 // PIECE
    halves = []
    for half in range(PAIR):
        halves.append(
            jnp.concatenate([grads_ref[PAIR * i + half] for i in range(pieces)], axis=0)
        )
    rest = rows - 2 * width
    folds = width // rest
    group = HALF // folds
    for part in range(2):
        both = jnp.concatenate([h[part * HALF : (part + 1) * HALF] for h in halves], axis=0)
        grad_ref[part * width : (part + 1) * width] = both.T
    tails = []
    for h in halves:
        tail = h[2 * HALF :]
        for fold in range(folds):
            tails.append(pltpu.roll(tail, width - fold * rest, 1) if fold else tail)
    assert len(tails) * group == width
    grad_ref[2 * width :] = jnp.concatenate(tails, axis=0).T[:rest]
    weight_grad = grad_ref[...] / math.sqrt(cells_all)
    moment_next = 0.9 * moment_ref[...] + 0.1 * weight_grad
    second_next = 0.999 * second_ref[...] + 0.001 * weight_grad * weight_grad
    master = master_ref[...]
    out_ref[...] = master - 0.001 * (moment_next / (jnp.sqrt(second_next) + 1e-08) + 0.01 * master)
    out_m_ref[...] = moment_next
    out_s_ref[...] = second_next


def exchanged(tiles, groups):
    return lax.all_to_all(tiles, "spatial", 0, 0, tiled=True, axis_index_groups=groups)


def moved(value, perm):
    return lax.ppermute(value, "spatial", perm)


def layer(volume, cotangent, master, moment, second):
    _, planes, rows, cols, width = volume.shape
    cells = rows * cols
    owners = lax.axis_size("dp")
    count = lax.axis_size("spatial")
    shard = master.shape[0]
    taps_all = owners * shard
    like = jax.ShapeDtypeStruct

    def inside(pairs):
        return [(i, j) for i, j in pairs if 0 <= j < count]

    swap = [(i, i ^ 1) for i in range(count)]
    outward = inside((i, i - 1 if i % 2 == 0 else i + 1) for i in range(count))

    packed = like((owners, shard // 2, width), BF16)
    send = pl.pallas_call(
        pack_body,
        out_shape=packed,
        name="pack",
        compiler_params=pltpu.CompilerParams(vmem_limit_bytes=8 << 20),
    )(master)
    halves = lax.all_to_all(send, "dp", 0, 0, tiled=True)
    edge, slab = pl.pallas_call(
        edges_body,
        out_shape=(like((3, rows, cols, width), BF16), like((4, rows, cols, width), BF16)),
        name="edges",
        compiler_params=pltpu.CompilerParams(vmem_limit_bytes=4 << 20),
    )(volume, cotangent)
    near = moved(edge, outward)
    whole = jnp.concatenate([v.reshape(-1, width) for v in (halves, near, slab)], axis=0)
    got = moved(whole, swap)
    activation, grad, weight = pl.pallas_call(
        forward_body,
        out_shape=(like(volume.shape, BF16), like((4 * cells, width), BF16), packed),
        scratch_shapes=[
            pltpu.VMEM((7 * cells, 9 * width), BF16),
            pltpu.VMEM((9 * width, 2 * width), BF16),
            pltpu.VMEM((9 * width, width), BF16),
            pltpu.VMEM((width, 4 * cells), F32),
            pltpu.VMEM((3 * HALF, 6 * cells), BF16),
            pltpu.VMEM((HALF, taps_all), F32),
        ],
        name="forward",
        compiler_params=pltpu.CompilerParams(vmem_limit_bytes=28 << 20),
    )(halves, got, volume, cotangent, near)
    arrived = lax.all_to_all(weight, "dp", 0, 0, tiled=True)
    input_grad = pl.pallas_call(
        backward_body,
        out_shape=like(volume.shape, BF16),
        scratch_shapes=[
            pltpu.VMEM((4 * cells, 9 * width), BF16),
            pltpu.VMEM((taps_all, width), BF16),
        ],
        cost_estimate=pl.CostEstimate(
            flops=2 * 2 * cells * taps_all * width, bytes_accessed=taps_all * width, transcendentals=0
        ),
        name="backward",
    compiler_params=pltpu.CompilerParams(vmem_limit_bytes=20 << 20),
    )(halves, got, grad)

    same_y = [
        [(y * MIDDLE + h) * PAIR + c for h in range(MIDDLE)] for y in range(OUTER) for c in range(PAIR)
    ]
    same_rest = [[y * MIDDLE * PAIR + r for y in range(OUTER)] for r in range(MIDDLE * PAIR)]
    same_z = [
        [(y * MIDDLE + h) * PAIR + c for y in range(OUTER) for c in range(PAIR)] for h in range(MIDDLE)
    ]
    pieces = shard // 2 // PIECE
    summed = arrived.astype(F32).sum(axis=0).reshape(pieces, PIECE, width)
    summed = jnp.pad(summed, ((0, OUTER - pieces), (0, 0), (0, 0)))
    piece = exchanged(summed, same_rest)
    piece = piece.sum(0)
    piece = exchanged(jnp.broadcast_to(piece[None], (MIDDLE, PIECE, width)), same_y)
    piece = piece.sum(0)
    joined = exchanged(jnp.broadcast_to(piece[None], (OUTER * PAIR, PIECE, width)), same_z)
    cells_all = owners * count * planes * cells
    state = like(master.shape, F32)
    master_next, moment_next, second_next = pl.pallas_call(
        functools.partial(update_body, cells_all),
        out_shape=(state, state, state),
        scratch_shapes=[pltpu.VMEM(master.shape, F32)],
        name="update",
        compiler_params=pltpu.CompilerParams(vmem_limit_bytes=8 << 20),
    )(joined, master, moment, second)
    return (activation, input_grad, master_next, moment_next, second_next)


def solution(mesh):
    return jax.shard_map(
        layer,
        mesh=mesh,
        in_specs=(
            P("dp", "spatial", None, None, None),
            P("dp", "spatial", None, None, None),
            P("dp", None),
            P("dp", None),
            P("dp", None),
        ),
        out_specs=(
            P("dp", "spatial", None, None, None),
            P("dp", "spatial", None, None, None),
            P("dp", None),
            P("dp", None),
            P("dp", None),
        ),
        check_vma=False,
    )
```

```python
import functools
import math

import jax
import jax.numpy as jnp
from jax import lax
from jax.experimental import pallas as pl
from jax.experimental.pallas import tpu as pltpu
from jax.sharding import PartitionSpec as P

F32 = jnp.float32
BF16 = jnp.bfloat16
OUTER = 8
MIDDLE = 4
PAIR = 2
HALF = 64
PIECE = 24


def core_is_low():
    return lax.rem(lax.axis_index("spatial"), PAIR) == 0


def lane_of(shape):
    return lax.broadcasted_iota(jnp.int32, shape, len(shape) - 1)


def pick(low, when_low, when_high):
    return jnp.where(low, when_low, when_high)


def pack_body(master_ref, send_ref, rows_ref, packed_ref, in_sem, out_sems):
    low = core_is_low()
    fetch = pltpu.make_async_copy(master_ref, rows_ref, in_sem)
    fetch.start()
    fetch.wait()
    rows = rows_ref.shape[0] // 2
    top = rows_ref[:rows]
    bottom = rows_ref[rows:]
    first = pick(low, top, pltpu.roll(top, HALF, 1))
    second = pick(low, pltpu.roll(bottom, HALF, 1), bottom)
    packed_ref[...] = jnp.where(lane_of(top.shape) < HALF, first, second).astype(BF16)
    copies = [
        pltpu.make_async_copy(packed_ref, send_ref.at[owner], out_sems.at[owner])
        for owner in range(send_ref.shape[0])
    ]
    for copy in copies:
        copy.start()
    for copy in copies:
        copy.wait()


def edges_body(volume_ref, cot_ref, near_ref, slab_ref):
    low = core_is_low()
    near_ref[:2] = volume_ref[0]
    near_ref[2] = pick(low, cot_ref[0, 0].astype(F32), cot_ref[0, 1].astype(F32)).astype(BF16)
    slab_ref[:2] = volume_ref[0]
    slab_ref[2:] = cot_ref[0]


def shifted(plane, dy, dx):
    _, cols, width = plane.shape
    if dx:
        at = lax.broadcasted_iota(jnp.int32, plane.shape, 1)
        keep = at < cols - 1 if dx > 0 else at > 0
        plane = jnp.where(keep, pltpu.roll(plane, (-dx) % cols, 1), 0.0)
    if dy:
        gap = jnp.zeros((1, cols, width), plane.dtype)
        plane = jnp.concatenate([plane[1:], gap] if dy > 0 else [gap, plane[:-1]], axis=0)
    return plane


def tap_pieces(plane, sign):
    columns = [shifted(plane, 0, sign * (f - 1)) for f in range(3)]
    return [shifted(columns[f], sign * (e - 1), 0) for e in range(3) for f in range(3)]


def kernel_rows(low, mine, other):
    mine = mine.astype(F32)
    other = other.astype(F32)
    left = pick(low, mine, other)
    right = pick(low, other, mine)
    keep = lane_of(left.shape) < HALF
    first = jnp.where(keep, left, pltpu.roll(right, HALF, 1))
    second = jnp.where(keep, pltpu.roll(left, HALF, 1), right)
    return first.astype(BF16), second.astype(BF16)


def forward_body(
    kernel_ref,
    got_ref,
    volume_ref,
    cot_ref,
    near_ref,
    out_act_ref,
    grad_ref,
    weight_ref,
    window_ref,
    wide_ref,
    deep_ref,
    turned_ref,
    stack_ref,
    total_ref,
):
    low = core_is_low()
    owners, rows, width = kernel_ref.shape
    shape = volume_ref.shape[2:]
    cells = shape[0] * shape[1]
    halves = owners * rows

    def handed(index):
        return got_ref[halves + index * cells : halves + (index + 1) * cells].astype(F32).reshape(shape)

    own = [volume_ref[0, i].astype(F32) for i in range(2)]
    near = [near_ref[i].astype(F32) for i in range(3)]
    far = [handed(i) for i in range(3)]
    beside = [handed(3 + i) for i in range(4)]
    low_planes = [*near[:2], *own, *beside[:2], far[0]]
    high_planes = [far[1], *beside[:2], *own, *near[:2]]
    planes = [pick(low, x, y) for x, y in zip(low_planes, high_planes)]
    for index, plane in enumerate(planes):
        for tap, piece in enumerate(tap_pieces(plane, 1)):
            window_ref[index * cells : (index + 1) * cells, tap * width : (tap + 1) * width] = (
                piece.reshape(cells, width).astype(BF16)
            )
    cot_own = [cot_ref[0, i].astype(F32) for i in range(2)]
    cots = [pick(low, x, y) for x, y in zip([near[2], *cot_own, *beside[2:]], [*beside[2:], *cot_own, near[2]])]
    cotangent = jnp.concatenate([c.reshape(cells, width) for c in cots], axis=0)
    group = owners // 3
    for owner in range(owners):
        offset, j = divmod(owner, group)
        blocks = kernel_rows(low, kernel_ref[owner], got_ref[owner * rows : (owner + 1) * rows])
        for k in range(2):
            at = slice((2 * j + k) * rows, (2 * j + k + 1) * rows)
            if offset < 2:
                wide_ref[at, offset * width : (offset + 1) * width] = blocks[k]
            else:
                deep_ref[at] = blocks[k]
    count = 5 * cells
    inner = 4 * cells
    span = 9 * width
    product = jnp.dot(window_ref[: count + cells], wide_ref[...], preferred_element_type=F32)
    part = count // 2
    preact = jnp.concatenate(
        [
            jnp.dot(
                window_ref[2 * cells + i * part : 2 * cells + (i + 1) * part],
                deep_ref[...],
                preferred_element_type=F32,
            )
            for i in range(2)
        ],
        axis=0,
    )
    preact = preact + product[:count, :width] + product[cells:, width:]
    sigma = jax.nn.sigmoid(preact)
    slope = sigma * (1.0 + preact * (1.0 - sigma))
    act = (preact * sigma)[cells : 4 * cells]
    act = pick(low, act[: inner // 2], act[cells:])
    out_act_ref[0] = act.reshape(out_act_ref.shape[1:]).astype(BF16)
    grad = cotangent * slope
    grad_ref[...] = pick(low, grad[:inner], grad[cells:]).astype(BF16)
    turned_ref[...] = pick(low, grad[cells:], grad[:inner]).T
    mine = pick(low, turned_ref[:HALF], turned_ref[HALF:]).astype(BF16)
    stack_ref[...] = jnp.zeros_like(stack_ref)
    for offset in range(3):
        stack_ref[offset * HALF : (offset + 1) * HALF, offset * cells : offset * cells + inner] = mine
    at = pl.multiple_of(jnp.where(low, cells, 0), cells)
    for left, right in ((0, 5 * width), (5 * width, span)):
        stacked = jnp.dot(
            stack_ref[...], window_ref[pl.ds(at, 6 * cells), left:right], preferred_element_type=F32
        )
        for offset in range(3):
            total_ref[:, offset * span + left : offset * span + right] = stacked[
                offset * HALF : (offset + 1) * HALF
            ]
    lane = lane_of((HALF, width))

    def columns(start):
        tile, offset = divmod(start, width)
        here = total_ref[:, tile * width : (tile + 1) * width]
        if not offset:
            return here
        here = pltpu.roll(here, width - offset, 1)
        if (tile + 1) * width >= total_ref.shape[1]:
            return here
        after = pltpu.roll(total_ref[:, (tile + 1) * width : (tile + 2) * width], width - offset, 1)
        return jnp.where(lane < width - offset, here, after)

    shard = 2 * rows
    rest = shard - 2 * width
    folds = width // rest
    lines = HALF // folds
    for owner in range(owners):
        start = owner * shard
        weight_ref[owner, :HALF] = columns(start).astype(BF16)
        weight_ref[owner, HALF : 2 * HALF] = columns(start + width).astype(BF16)
        tail = columns(start + 2 * width)
        folded = tail[:lines]
        for fold in range(1, folds):
            part = pltpu.roll(tail[fold * lines : (fold + 1) * lines], fold * rest, 1)
            folded = jnp.where(lane[:lines] >= fold * rest, part, folded)
        weight_ref[owner, 2 * HALF :] = folded.astype(BF16)


def backward_body(kernel_ref, got_ref, grad_ref, out_ref, window_ref, turn_ref):
    low = core_is_low()
    owners, rows, width = kernel_ref.shape
    shape = out_ref.shape[2:]
    cells = grad_ref.shape[0] // 4
    for owner in range(owners):
        blocks = kernel_rows(low, kernel_ref[owner], got_ref[owner * rows : (owner + 1) * rows])
        for k in range(2):
            turn_ref[(2 * owner + k) * rows : (2 * owner + k + 1) * rows] = blocks[k]
    for index in range(4):
        plane = grad_ref[index * cells : (index + 1) * cells].astype(F32).reshape(shape)
        for tap, piece in enumerate(tap_pieces(plane, -1)):
            window_ref[index * cells : (index + 1) * cells, tap * width : (tap + 1) * width] = (
                piece.reshape(cells, width).astype(BF16)
            )
    total = jnp.zeros((2 * cells, width), F32)
    for offset in range(3):
        for tap in range(9):
            at = (offset * 9 + tap) * width
            total = total + lax.dot_general(
                window_ref[(2 - offset) * cells : (4 - offset) * cells, tap * width : (tap + 1) * width],
                turn_ref[at : at + width],
                (((1,), (1,)), ((), ())),
                preferred_element_type=F32,
            )
    out_ref[0] = total.reshape(2, *shape).astype(BF16)


def update_body(cells_all, grads_ref, master_ref, moment_ref, second_ref, out_ref, out_m_ref, out_s_ref, grad_ref):
    rows, width = master_ref.shape
    pieces = rows // 2 // PIECE
    halves = []
    for half in range(PAIR):
        halves.append(
            jnp.concatenate([grads_ref[PAIR * i + half] for i in range(pieces)], axis=0)
        )
    rest = rows - 2 * width
    folds = width // rest
    group = HALF // folds
    for part in range(2):
        both = jnp.concatenate([h[part * HALF : (part + 1) * HALF] for h in halves], axis=0)
        grad_ref[part * width : (part + 1) * width] = both.T
    tails = []
    for h in halves:
        tail = h[2 * HALF :]
        for fold in range(folds):
            tails.append(pltpu.roll(tail, width - fold * rest, 1) if fold else tail)
    assert len(tails) * group == width
    grad_ref[2 * width :] = jnp.concatenate(tails, axis=0).T[:rest]
    weight_grad = grad_ref[...] / math.sqrt(cells_all)
    moment_next = 0.9 * moment_ref[...] + 0.1 * weight_grad
    second_next = 0.999 * second_ref[...] + 0.001 * weight_grad * weight_grad
    master = master_ref[...]
    out_ref[...] = master - 0.001 * (moment_next / (jnp.sqrt(second_next) + 1e-08) + 0.01 * master)
    out_m_ref[...] = moment_next
    out_s_ref[...] = second_next


def exchanged(tiles, groups):
    return lax.all_to_all(tiles, "spatial", 0, 0, tiled=True, axis_index_groups=groups)


def moved(value, perm):
    return lax.ppermute(value, "spatial", perm)


def layer(volume, cotangent, master, moment, second):
    _, planes, rows, cols, width = volume.shape
    cells = rows * cols
    owners = lax.axis_size("dp")
    count = lax.axis_size("spatial")
    shard = master.shape[0]
    taps_all = owners * shard
    like = jax.ShapeDtypeStruct

    def inside(pairs):
        return [(i, j) for i, j in pairs if 0 <= j < count]

    swap = [(i, i ^ 1) for i in range(count)]
    outward = inside((i, i - 1 if i % 2 == 0 else i + 1) for i in range(count))

    packed = like((owners, shard // 2, width), BF16)
    send = pl.pallas_call(
        pack_body,
        out_shape=packed,
        in_specs=[pl.BlockSpec(memory_space=pltpu.HBM)],
        out_specs=pl.BlockSpec(memory_space=pltpu.HBM),
        scratch_shapes=[
            pltpu.VMEM(master.shape, F32),
            pltpu.VMEM(packed.shape[1:], BF16),
            pltpu.SemaphoreType.DMA,
            pltpu.SemaphoreType.DMA((owners,)),
        ],
        name="pack",
        compiler_params=pltpu.CompilerParams(vmem_limit_bytes=8 << 20),
    )(master)
    halves = lax.all_to_all(send, "dp", 0, 0, tiled=True)
    edge, slab = pl.pallas_call(
        edges_body,
        out_shape=(like((3, rows, cols, width), BF16), like((4, rows, cols, width), BF16)),
        name="edges",
        compiler_params=pltpu.CompilerParams(vmem_limit_bytes=4 << 20),
    )(volume, cotangent)
    near = moved(edge, outward)
    whole = jnp.concatenate([v.reshape(-1, width) for v in (halves, near, slab)], axis=0)
    got = moved(whole, swap)
    activation, grad, weight = pl.pallas_call(
        forward_body,
        out_shape=(like(volume.shape, BF16), like((4 * cells, width), BF16), packed),
        scratch_shapes=[
            pltpu.VMEM((7 * cells, 9 * width), BF16),
            pltpu.VMEM((9 * width, 2 * width), BF16),
            pltpu.VMEM((9 * width, width), BF16),
            pltpu.VMEM((width, 4 * cells), F32),
            pltpu.VMEM((3 * HALF, 6 * cells), BF16),
            pltpu.VMEM((HALF, taps_all), F32),
        ],
        name="forward",
        compiler_params=pltpu.CompilerParams(vmem_limit_bytes=28 << 20),
    )(halves, got, volume, cotangent, near)
    arrived = lax.all_to_all(weight, "dp", 0, 0, tiled=True)
    input_grad = pl.pallas_call(
        backward_body,
        out_shape=like(volume.shape, BF16),
        scratch_shapes=[
            pltpu.VMEM((4 * cells, 9 * width), BF16),
            pltpu.VMEM((taps_all, width), BF16),
        ],
        cost_estimate=pl.CostEstimate(
            flops=2 * 2 * cells * taps_all * width, bytes_accessed=taps_all * width, transcendentals=0
        ),
        name="backward",
    compiler_params=pltpu.CompilerParams(vmem_limit_bytes=20 << 20),
    )(halves, got, grad)

    same_y = [
        [(y * MIDDLE + h) * PAIR + c for h in range(MIDDLE)] for y in range(OUTER) for c in range(PAIR)
    ]
    same_rest = [[y * MIDDLE * PAIR + r for y in range(OUTER)] for r in range(MIDDLE * PAIR)]
    same_z = [
        [(y * MIDDLE + h) * PAIR + c for y in range(OUTER) for c in range(PAIR)] for h in range(MIDDLE)
    ]
    pieces = shard // 2 // PIECE
    summed = arrived.astype(F32).sum(axis=0).reshape(pieces, PIECE, width)
    summed = jnp.pad(summed, ((0, OUTER - pieces), (0, 0), (0, 0)))
    piece = exchanged(summed, same_rest)
    piece = piece.sum(0)
    piece = exchanged(jnp.broadcast_to(piece[None], (MIDDLE, PIECE, width)), same_y)
    piece = piece.sum(0)
    joined = exchanged(jnp.broadcast_to(piece[None], (OUTER * PAIR, PIECE, width)), same_z)
    cells_all = owners * count * planes * cells
    state = like(master.shape, F32)
    master_next, moment_next, second_next = pl.pallas_call(
        functools.partial(update_body, cells_all),
        out_shape=(state, state, state),
        scratch_shapes=[pltpu.VMEM(master.shape, F32)],
        name="update",
        compiler_params=pltpu.CompilerParams(vmem_limit_bytes=8 << 20),
    )(joined, master, moment, second)
    return (activation, input_grad, master_next, moment_next, second_next)


def solution(mesh):
    return jax.shard_map(
        layer,
        mesh=mesh,
        in_specs=(
            P("dp", "spatial", None, None, None),
            P("dp", "spatial", None, None, None),
            P("dp", None),
            P("dp", None),
            P("dp", None),
        ),
        out_specs=(
            P("dp", "spatial", None, None, None),
            P("dp", "spatial", None, None, None),
            P("dp", None),
            P("dp", None),
            P("dp", None),
        ),
        check_vma=False,
    )
```
